32 devices in a mesh: gx: 4 (over y, core), gy: 8 (over z, x).
Axes of the slice: x: 2, y: 2, z: 4, core: 2. Of those that a mesh axis runs over, the one named last changes fastest.
Arguments:
- source: float32 [64, 16, 1024], P(None, 'gx', 'gy'), may hold values from -6 to 6
- initial: float32 [64, 16, 1024], P(None, 'gx', 'gy'), may hold values from -6 to 6
- reaction: float32 [64, 16, 1024], P(None, 'gx', 'gy'), may hold values from 1 to 3
- stiffness: float32 [16, 1024], P('gx', 'gy'), may hold values from 0.5 to 2
- line_op: float32 [8, 8], replicated, may hold values from -1.6 to 5.6
- face_deriv: float32 [8], replicated, may hold values from -2 to 2
- wall_flags: int32 [4, 16, 1024], P(None, 'gx', 'gy'), may hold values 0 or 1
Outputs:
- hessenberg: float32 [6, 5], replicated
- krylov_basis: float32 [6, 64, 16, 1024], P(None, None, 'gx', 'gy')
The draws below stay inside these ranges and needn't reach their ends.
All inputs are finite; a program needn't handle non-finite values. No bound on the sum of `wall_flags` on one device may be relied on, other than what follows from the above.
Results may differ from the reference program's by a relative error of at most 0.0003.
Values sent between devices are 32-bit elements; how exact they have to be, the bound alone decides.
A program may use at most 64 MiB of HBM per device.

```python
import math
import jax
import jax.numpy as jnp
from jax import lax

P_SIZE = 8
ITERS = 5
NEX = 16
NEY = 1024


def draw_line_op(key, part):
    first_key, second_key = jax.random.split(jax.random.fold_in(key, 11))
    offdiag = jnp.clip(jax.random.normal(first_key, (P_SIZE, P_SIZE), jnp.float32) * 0.4, -1.6, 1.6)
    diagonal = jax.random.uniform(second_key, (P_SIZE,), jnp.float32, 2.0, 4.0)
    return offdiag * (1.0 - jnp.eye(P_SIZE, dtype=jnp.float32)) + jnp.diag(diagonal)


def place_ends(values, rng, least, largest):
    longest = values.shape.index(max(values.shape))
    spots = []
    for shift in (0, 1):
        where = [jax.random.randint(jax.random.fold_in(rng, axis), (), 0, length) for axis, length in enumerate(values.shape)]
        where[longest] = (where[longest] + shift) % values.shape[longest]
        spots.append(tuple(where))
    return values.at[spots[0]].set(least).at[spots[1]].set(largest)


def block_scale(rng, extent, cuts, low, largest):
    def one(position, shards_of):
        draws = jax.random.uniform(jax.random.fold_in(jax.random.fold_in(rng, 6), position), (shards_of,), jnp.float32, low / len(cuts), largest / len(cuts))
        return jnp.repeat(jnp.exp(draws), extent[position] // shards_of).reshape((-1,) + (1,) * (len(extent) - position - 1))

    factor_of = one(*cuts[0])
    for cut in cuts[1:]:
        factor_of = factor_of * one(*cut)
    return factor_of


def gaussian(rng, extent, deviation, most, cuts=(), held_as=jnp.bfloat16):
    values = deviation * jax.random.normal(rng, extent, jnp.float32)
    if cuts:
        values = values * block_scale(rng, extent, cuts, -0.22, 0.18)
    return jnp.clip(values, -most, most).astype(held_as)


def setup_inputs(seed: int = 0) -> dict:
    streams_of = jax.random.split(jax.random.key(seed), 8)
    source = gaussian(streams_of[0], (P_SIZE * P_SIZE, NEX, NEY), 1.0, 6.0, ((1, 4), (2, 8)), jnp.float32)
    initial = gaussian(streams_of[1], (P_SIZE * P_SIZE, NEX, NEY), 1.0, 6.0, ((1, 4), (2, 8)), jnp.float32)
    reaction = jnp.clip(1.0 + 2.0 * jax.random.uniform(streams_of[2], (P_SIZE * P_SIZE, NEX, NEY), jnp.float32) ** block_scale(streams_of[2], (P_SIZE * P_SIZE, NEX, NEY), ((1, 4), (2, 8)), -0.2, 0.2), 1.0, 3.0)
    stiffness = jnp.clip(jnp.exp(math.log(2.0) - 1.3862944 * jax.random.uniform(streams_of[3], (NEX, NEY), jnp.float32) ** block_scale(streams_of[3], (NEX, NEY), ((0, 4), (1, 8)), -0.2, 0.2)), 0.5, 2.0)
    line_op = draw_line_op(jax.random.fold_in(streams_of[7], 71), 0)
    face_deriv = gaussian(streams_of[5], (P_SIZE,), 0.5, 2.0, (), jnp.float32)
    wall_flags = place_ends((jax.random.randint(streams_of[6], (4, NEX, NEY), 0, 4) < 1).astype(jnp.int32), jax.random.fold_in(streams_of[6], 1), 0, 1)
    return {"source": source, "initial": initial, "reaction": reaction, "stiffness": stiffness, "line_op": line_op, "face_deriv": face_deriv, "wall_flags": wall_flags}


TAU = 2.0
FLOOR = 0.1

def block_sum(values):
    flat = values.reshape(-1)
    width = 1024
    extra = -flat.shape[0] % width
    flat = jnp.concatenate([flat, jnp.zeros((extra,), flat.dtype)])
    return jnp.sum(lax.optimization_barrier(jnp.sum(flat.reshape(-1, width), axis=1)))

def apply_op(field, reaction, stiffness, line_op, face_deriv, wall_flags):
    highest = lax.Precision.HIGHEST
    nodes = field.reshape(P_SIZE, P_SIZE, field.shape[1], field.shape[2])
    interior = stiffness * (jnp.einsum('ac,cbxy->abxy', line_op, nodes, precision=highest) + jnp.einsum('bc,acxy->abxy', line_op, nodes, precision=highest))
    reversed_w = face_deriv[::-1]
    west_val = nodes[0]
    east_val = nodes[P_SIZE - 1]
    south_val = nodes[:, 0]
    north_val = nodes[:, P_SIZE - 1]
    west_der = jnp.einsum('c,cbxy->bxy', face_deriv, nodes, precision=highest)
    east_der = jnp.einsum('c,cbxy->bxy', reversed_w, nodes, precision=highest)
    south_der = jnp.einsum('c,acxy->axy', face_deriv, nodes, precision=highest)
    north_der = jnp.einsum('c,acxy->axy', reversed_w, nodes, precision=highest)
    opened = 1.0 - wall_flags.astype(field.dtype)
    add_east = TAU * (east_val - opened[1] * jnp.roll(west_val, -1, 1)) + 0.5 * (east_der - opened[1] * jnp.roll(west_der, -1, 1))
    add_west = TAU * (west_val - opened[0] * jnp.roll(east_val, 1, 1)) + 0.5 * (west_der - opened[0] * jnp.roll(east_der, 1, 1))
    add_north = TAU * (north_val - opened[3] * jnp.roll(south_val, -1, 2)) + 0.5 * (north_der - opened[3] * jnp.roll(south_der, -1, 2))
    add_south = TAU * (south_val - opened[2] * jnp.roll(north_val, 1, 2)) + 0.5 * (south_der - opened[2] * jnp.roll(north_der, 1, 2))
    result = reaction.reshape(nodes.shape) * nodes + interior
    result = result.at[0].add(add_west).at[P_SIZE - 1].add(add_east)
    result = result.at[:, 0].add(add_south).at[:, P_SIZE - 1].add(add_north)
    return result.reshape(field.shape)

def reference(source, initial, reaction, stiffness, line_op, face_deriv, wall_flags):
    total = float(P_SIZE * P_SIZE * NEX * NEY)

    def operate(field):
        return apply_op(field, reaction, stiffness, line_op, face_deriv, wall_flags)
    first = source - operate(initial)
    beta_first = jnp.sqrt(block_sum(first * first) / total + FLOOR)
    vectors = [first / beta_first]
    hessen = jnp.zeros((ITERS + 1, ITERS), source.dtype)
    for step in range(ITERS):
        image = operate(vectors[step])
        coeffs = [block_sum(vector * image) / total for vector in vectors]
        for index in range(len(vectors)):
            image = image - coeffs[index] * vectors[index]
            hessen = hessen.at[index, step].set(coeffs[index])
        beta = jnp.sqrt(block_sum(image * image) / total + FLOOR)
        hessen = hessen.at[step + 1, step].set(beta)
        vectors.append(image / beta)
    return (hessen, jnp.stack(vectors))
```

```python
import functools

import jax
import jax.numpy as jnp
from jax import lax
from jax.experimental import pallas as pl
from jax.experimental.pallas import tpu as pltpu
from jax.sharding import PartitionSpec as P

P_SIZE = 8
ITERS = 5
VECS = ITERS + 1
TAU = 2.0
FLOOR = 0.1
PAIRS = P_SIZE // 2
SLOT = 32
GHOST = 8
WIDE = 3 * P_SIZE + 4
NARROW = 3 * 2 + 1
MESH = pl.DeviceIdType.MESH


def block_offsets(nx):
    near = min(nx, 5)
    return list(range(-((near - 1) // 2), near // 2 + 1))


def kernel(
    nx, ny, total,
    line, deriv, src_any, ini_any, rea_any, stf, wal,
    hess_out, bas,
    coef, gcoef, scoef, sgcoef, small, src, ini, rea,
    wide, low_send, high_send, south_in, north_in,
    page_ini, page_src, page_rea, page_small, page_a, page_b, patch,
    in_sem, hsend, hrecv, rsend, rrecv,
    hs_sem, hr_sem, ws_sem, wr_sem, ns_sem, nr_sem, rs_sem, rr_sem,
):
    n = nx * ny
    offs = block_offsets(nx)
    blocks = len(offs)
    here = offs.index(0)
    gx, gy = lax.axis_index("gx"), lax.axis_index("gy")
    me = gx * ny + gy

    side = gy // (ny // 2)
    offsets = sorted(range(1, nx), key=lambda d: abs(2 * d - nx))

    def for_peers(act):
        def column(k, own_column):
            across = side * k + (1 - side) * (ny - 1 - k)
            for d in offsets:
                act((lax.rem(gx + d, nx), across))
            if own_column:
                skip = jnp.where(k >= (side * gy + (1 - side) * (ny - 1 - gy)), 1, 0)
                act((gx, across + (2 * side - 1) * skip))

        if n <= 64:
            for k in range(ny - 1):
                column(k, True)
        else:
            lax.fori_loop(0, ny - 1, lambda k, c: (column(k, True), c)[1], 0)
        column(ny - 1, False)

    def at(dx, dy):
        return (lax.rem(gx + dx + nx, nx), lax.rem(gy + dy + ny, ny))

    barrier = pltpu.get_barrier_semaphore()

    def greet(device):
        pl.semaphore_signal(barrier, inc=1, device_id=device, device_id_type=MESH)

    loads = [
        pltpu.make_async_copy(given, held, in_sem.at[k])
        for k, (given, held) in enumerate(((ini_any, ini), (src_any, src), (rea_any, rea)))
    ]
    for load in loads:
        load.start()
    for_peers(greet)

    sub = lax.broadcasted_iota(jnp.int32, (8, 128), 0)
    lane = lax.broadcasted_iota(jnp.int32, (8, 128), 1)
    low = sub < 4
    xpos = sub % 4
    slot_of = lane // SLOT
    in_slot = lane % SLOT
    south_half = in_slot < SLOT // 2
    group_of = in_slot // GHOST

    def srl(v, s):
        s = s % 8
        return v if s == 0 else pltpu.roll(v, s, 0)

    def lrl(v, s):
        s = s % 128
        return v if s == 0 else pltpu.roll(v, s, 1)

    def halves(a, b):
        return jnp.where(low, a, b)

    def by_slot(parts):
        out = parts[0]
        for p in range(1, PAIRS):
            out = jnp.where(slot_of == p, parts[p], out)
        return out

    def dot(pairs):
        out = None
        for c, v in pairs:
            out = c * v if out is None else out + c * v
        return out

    mix = {}
    for p in range(PAIRS):
        for r in range(PAIRS):
            mix[p, r, 0] = halves(line[2 * p, 2 * r], line[2 * p + 1, 2 * r + 1])
            mix[p, r, 1] = halves(line[2 * p, 2 * r + 1], line[2 * p + 1, 2 * r])
            for k in range(2):
                coef[(p * PAIRS + r) * 2 + k] = mix[p, r, k]
    glow = [0.5 * deriv[c] + (TAU if c == 0 else 0.0) for c in range(P_SIZE)]
    gupp = [
        0.5 * deriv[P_SIZE - 1 - c] + (TAU if c == P_SIZE - 1 else 0.0) for c in range(P_SIZE)
    ]
    lows = [halves(glow[2 * p], glow[2 * p + 1]) for p in range(PAIRS)]
    upps = [halves(gupp[2 * p], gupp[2 * p + 1]) for p in range(PAIRS)]
    for p in range(PAIRS):
        gcoef[p] = lows[p]
        gcoef[PAIRS + p] = upps[p]
    small[0, 0:4] = stf[...]
    small[0, 4:8] = stf[...]
    opened = [1.0 - wal[f].astype(jnp.float32) for f in range(4)]
    for slot, (first, second) in enumerate(((0, 0), (1, 1), (2, 3))):
        small[slot + 1, 0:4] = opened[first]
        small[slot + 1, 4:8] = opened[second]
    trace = line[0, 0]
    for c in range(1, P_SIZE):
        trace = trace + line[c, c]
    shift = 3.0 + 0.25 * trace

    def tile(ref, a, p):
        return ref[pl.ds((a * PAIRS + p) * 8, 8), :]

    def put(ref, a, p, value):
        ref[pl.ds((a * PAIRS + p) * 8, 8), :] = value

    def tiles():
        return [(a, p) for a in range(P_SIZE) for p in range(PAIRS)]

    def xfaces(get):
        fw, fe = [], []
        for p in range(PAIRS):
            vs = [get(c, p) for c in range(P_SIZE)]
            fw.append(dot(zip(glow, vs)))
            fe.append(dot(zip(gupp, vs)))
        return fw, fe

    def halo_copy(slot, way, device):
        return pltpu.make_async_remote_copy(
            src_ref=hsend.at[slot, way],
            dst_ref=hrecv.at[slot, way],
            send_sem=hs_sem.at[slot, way],
            recv_sem=hr_sem.at[slot, way],
            device_id=device,
            device_id_type=MESH,
        )

    def send_halo(slot, faces, ready=lambda: None):
        fw, fe = faces
        cw, ce = fw[0], srl(fe[0], -3)
        for p in range(1, PAIRS):
            cw = jnp.where(xpos == p, srl(fw[p], p), cw)
            ce = jnp.where(xpos == p, srl(fe[p], p - 3), ce)
        hsend[slot, 0] = cw
        hsend[slot, 1] = ce
        ready()
        copies = [halo_copy(slot, 0, at(-1, 0)), halo_copy(slot, 1, at(1, 0))]
        for copy in copies:
            copy.start()
        return copies

    def take_halo(slot, copies, sign):
        for copy in copies:
            copy.wait_recv()
        cw, ce = hrecv[slot, 0], hrecv[slot, 1]
        open_w, open_e = small[1] * sign, small[2] * sign
        first = [open_w * jnp.where(xpos == 0, srl(ce, -p), 0.0) for p in range(PAIRS)]
        last = [open_e * jnp.where(xpos == 3, srl(cw, 3 - p), 0.0) for p in range(PAIRS)]
        return first, last

    def operate(get, faces, moved, emit):
        fw, fe = faces
        stiff, open_w, open_e, open_y = small[0], small[1], small[2], small[3]
        sides = {}
        for p in range(PAIRS):
            nb_e = jnp.where(xpos == 3, 0.0, srl(fw[p], 7))
            nb_w = jnp.where(xpos == 0, 0.0, srl(fe[p], 1))
            sides[0, p] = fw[p] - open_w * nb_w
            sides[P_SIZE - 1, p] = fe[p] - open_e * nb_e
        for a in range(P_SIZE):
            vs = [get(a, p) for p in range(PAIRS)]
            ss = [srl(v, 4) for v in vs]
            s = dot((gcoef[p], vs[p]) for p in range(PAIRS))
            t = dot((gcoef[PAIRS + p], vs[p]) for p in range(PAIRS))
            own = halves(s, t) + srl(halves(t, s), 4)
            q = srl(own, 4)
            term = own - open_y * halves(lrl(q, 1), lrl(q, 127))
            for p in range(PAIRS):
                acc = None
                for r in range(PAIRS):
                    k = (p * PAIRS + r) * 2
                    part = coef[k] * vs[r] + coef[k + 1] * ss[r]
                    acc = part if acc is None else acc + part
                other = dot((line[a, c], get(c, p)) for c in range(P_SIZE))
                react = tile(rea, a, p) - shift if moved else tile(rea, a, p)
                value = react * vs[p] + stiff * (acc + other)
                if p == 0:
                    value = value + jnp.where(low, term, 0.0)
                if p == PAIRS - 1:
                    value = value + jnp.where(low, 0.0, term)
                if (a, p) in sides:
                    value = value + sides[a, p]
                emit(a, p, value)

    def gather_rows(accs):
        zero = jnp.zeros((8, 128), jnp.float32)
        level = list(accs) + [zero] * (8 - len(accs))
        for step in (1, 2, 4):
            keep = (sub // step) % 2 == 0
            level = [
                jnp.where(keep, level[i], level[i + 1])
                + srl(jnp.where(keep, level[i + 1], level[i]), step)
                for i in range(0, len(level), 2)
            ]
        return level[0]

    def fold(v):
        for step in (4, 2, 1):
            v = v + srl(v, step)
        return v

    def row_copy(slot, device):
        return pltpu.make_async_remote_copy(
            src_ref=rsend.at[slot],
            dst_ref=rrecv.at[slot, pl.ds(me, 1)],
            send_sem=rs_sem.at[slot],
            recv_sem=rr_sem.at[slot],
            device_id=device,
            device_id_type=MESH,
        )

    def pack_sums(accs, start):
        sums = jnp.sum(gather_rows(accs), axis=1, keepdims=True)
        return jnp.where(lane == sub + start, sums, 0.0)

    def start_reduce(slot, packed):
        row = fold(packed)[0:1]
        rsend[slot] = row
        rrecv[slot, pl.ds(me, 1)] = row
        for_peers(lambda device: row_copy(slot, device).start())

    def end_reduce(slot):
        block = rrecv.at[slot, pl.ds(0, n - 1)]
        pltpu.make_async_copy(block, block, rr_sem.at[slot]).wait()
        value = rrecv[slot, 0:8]
        for g in range(1, n // 8):
            value = value + rrecv[slot, 8 * g:8 * g + 8]
        value = fold(value)
        return lambda k: jnp.broadcast_to(value[:, k:k + 1], (8, 128))

    fields = ((ini, 0), (src, 1), (rea, 2))

    def narrow_copy(sent, held, back, dx, dy):
        j = offs.index(back)
        return pltpu.make_async_remote_copy(
            src_ref=sent,
            dst_ref=held.at[j],
            send_sem=ns_sem.at[0 if dy < 0 else 1, j],
            recv_sem=nr_sem.at[0 if dy < 0 else 1, j],
            device_id=at(dx, dy),
            device_id_type=MESH,
        )

    def opposite(o):
        return -o if -o in offs else o

    def wide_copy(o):
        j = offs.index(opposite(o))
        return pltpu.make_async_remote_copy(
            src_ref=wide.at[here],
            dst_ref=wide.at[j],
            send_sem=ws_sem.at[j],
            recv_sem=wr_sem.at[j],
            device_id=at(o, 0),
            device_id_type=MESH,
        )

    def pack_edges():
        def gathered(parts):
            return by_slot([lrl(parts[p], 16 + SLOT * p) for p in range(PAIRS)])

        def narrow(items, index):
            for ref, start in ((low_send, 16), (high_send, 8)):
                out = None
                for i, v in enumerate(items):
                    moved = lrl(v, GHOST * i - start)
                    out = moved if out is None else jnp.where(group_of == i, moved, out)
                ref[index] = out

        for ref, f in fields:
            for quad in range(2):
                items = []
                for a in range(4 * quad, 4 * quad + 4):
                    v = gathered([tile(ref, a, p) for p in range(PAIRS)])
                    wide[here, f * P_SIZE + a] = v
                    items.append(v)
                narrow(items, f * 2 + quad)
        items = []
        for f in range(4):
            v = gathered([small[f]] * PAIRS)
            wide[here, 3 * P_SIZE + f] = v
            items.append(v)
        narrow(items, 6)

    narrow_copies = [
        narrow_copy(low_send, north_in, opposite(o), o, -1) for o in offs
    ] + [
        narrow_copy(high_send, south_in, opposite(o), o, 1) for o in offs
    ]
    wide_copies = [wide_copy(o) for o in sorted(offs, key=abs) if o]

    for d in range(PAIRS):
        for k in range(2):
            scoef[2 * d + k] = by_slot([mix[(r + d) % PAIRS, r, k] for r in range(PAIRS)])
    sgcoef[0] = by_slot(lows)
    sgcoef[1] = by_slot(upps)
    y_mask = (low & (slot_of == 0)) | (~low & (slot_of == PAIRS - 1))

    def unpack_pages():
        def merge(seam, wide_part, narrow_part, i):
            if seam == 0:
                return jnp.where(south_half, lrl(narrow_part, GHOST - GHOST * i), wide_part)
            return jnp.where(south_half, wide_part, lrl(narrow_part, 16 - GHOST * i))

        for seam, narrow_in in ((0, south_in), (1, north_in)):
            for j in range(blocks):
                for f, page in enumerate((page_ini, page_src, page_rea)):
                    for a in range(P_SIZE):
                        page[seam, j * P_SIZE + a] = merge(
                            seam, wide[j, f * P_SIZE + a], narrow_in[j, f * 2 + a // 4], a % 4
                        )
                for f in range(4):
                    page_small[seam, j * 4 + f] = merge(
                        seam, wide[j, 3 * P_SIZE + f], narrow_in[j, 6], f
                    )

    def page_level(level):
        given = page_ini if level == 0 else (page_a if level % 2 else page_b)
        out = page_b if level % 2 else page_a

        def seam_body(seam, carry):
            fw, fe = [], []
            for j in range(blocks):
                vs = [given[seam, j * P_SIZE + a] for a in range(P_SIZE)]
                fw.append(dot(zip(glow, vs)))
                fe.append(dot(zip(gupp, vs)))
            for j in range(blocks):
                stiff, open_w, open_e, open_y = [page_small[seam, j * 4 + f] for f in range(4)]
                nb_e = jnp.where(xpos == 3, srl(fw[(j + 1) % blocks], 3), srl(fw[j], 7))
                nb_w = jnp.where(xpos == 0, srl(fe[(j - 1) % blocks], 5), srl(fe[j], 1))
                sides = {
                    0: fw[j] - open_w * nb_w,
                    P_SIZE - 1: fe[j] - open_e * nb_e,
                }
                vs = [given[seam, j * P_SIZE + a] for a in range(P_SIZE)]
                for a in range(P_SIZE):
                    v = vs[a]
                    ss = srl(v, 4)
                    acc = scoef[0] * v + scoef[1] * ss
                    for d in range(1, PAIRS):
                        acc = acc + lrl(scoef[2 * d] * v + scoef[2 * d + 1] * ss, SLOT * d)
                    s, t = sgcoef[0] * v, sgcoef[1] * v
                    own = halves(s, t) + srl(halves(t, s), 4)
                    own = own + lrl(own, 64)
                    own = own + lrl(own, 32)
                    q = srl(own, 4)
                    term = own - open_y * halves(lrl(q, 1), lrl(q, 127))
                    other = dot(zip([line[a, c] for c in range(P_SIZE)], vs))
                    react = page_rea[seam, j * P_SIZE + a]
                    if level:
                        react = react - shift
                    value = react * v + stiff * (acc + other) + jnp.where(y_mask, term, 0.0)
                    if a in sides:
                        value = value + sides[a]
                    if level == 0:
                        value = page_src[seam, j * P_SIZE + a] - value
                    out[seam, j * P_SIZE + a] = value
            return carry

        lax.fori_loop(0, 2, seam_body, 0)
        for a in range(P_SIZE):
            k = here * P_SIZE + a
            patch[level, a] = jnp.where(south_half, out[1, k], out[0, k])

    edge = (lane < VECS) | (lane >= 128 - VECS)

    def patched(level, a, p, v):
        return jnp.where(edge, lrl(patch[level, a], 112 - SLOT * p), v)

    started = []

    loads[0].wait()
    get = functools.partial(tile, ini)
    faces = xfaces(get)
    copies = send_halo(0, faces, lambda: pl.semaphore_wait(barrier, n - 1))
    started += copies
    loads[1].wait()
    loads[2].wait()
    y0 = bas.at[0]
    operate(get, faces, False, lambda a, p, v: put(y0, a, p, tile(src, a, p) - v))
    pack_edges()
    for copy in narrow_copies:
        copy.start()

    ways = len(wide_copies)
    for level in range(ITERS):
        now = bas.at[level]
        get = functools.partial(tile, now)
        fw, fe = xfaces(get)
        first, last = take_halo(level, copies, 1.0 if level == 0 else -1.0)
        fw = [fw[p] + glow[0] * first[p] + glow[P_SIZE - 1] * last[p] for p in range(PAIRS)]
        fe = [fe[p] + gupp[0] * first[p] + gupp[P_SIZE - 1] * last[p] for p in range(PAIRS)]
        copies = send_halo(level + 1, (fw, fe))
        started += copies
        for p in range(PAIRS):
            put(now, 0, p, get(0, p) + first[p])
            put(now, P_SIZE - 1, p, get(P_SIZE - 1, p) + last[p])
        operate(get, (fw, fe), True, functools.partial(put, bas.at[level + 1]))
        if level == 0:
            for copy in wide_copies[:ways - ways // 2]:
                copy.start()
        if level == 1:
            for copy in wide_copies[ways - ways // 2:]:
                copy.start()
            accs = [None] * 3
            for a, p in tiles():
                u, v = tile(bas.at[0], a, p), tile(bas.at[1], a, p)
                new = [u * u, u * v, v * v]
                accs = new if accs[0] is None else [s + t for s, t in zip(accs, new)]
            start_reduce(0, pack_sums(accs, 0))
        if level == 3:
            for copy in narrow_copies + wide_copies:
                copy.wait_recv()
            unpack_pages()
            for k in range(3):
                page_level(k)
        if level == 4:
            for k in range(3, VECS):
                page_level(k)

    sums = end_reduce(0)
    size = jnp.maximum(sums(0), 1e-30)
    mean = sums(1) / size
    spread = jnp.sqrt(jnp.maximum(sums(2) / size - mean * mean, 0.0)) + 0.1
    inv = 1.0 / spread
    ratio = mean * inv
    theta = shift + mean
    powers = [None, inv]
    for k in range(2, VECS):
        powers.append(powers[k - 1] * inv)

    pairs = [(i, j) for j in range(ITERS) for i in range(j + 1)]
    accs, tail = None, None
    for a, p in tiles():
        lev = []
        for k in range(VECS):
            v = patched(k, a, p, tile(bas.at[k], a, p))
            lev.append(v if k == 0 else v * powers[k])
        vecs = [lev[0]]
        for k in range(1, VECS):
            lev = [lev[i + 1] - ratio * lev[i] for i in range(len(lev) - 1)]
            vecs.append(lev[0])
        for k in range(1, VECS):
            put(bas.at[k], a, p, vecs[k])
        put(bas.at[0], a, p, vecs[0])
        new = [vecs[i] * vecs[j] for i, j in pairs]
        accs = new if accs is None else [s + t for s, t in zip(accs, new)]
        if 0 < a < P_SIZE - 1:
            new = [v * vecs[ITERS] for v in vecs]
            tail = new if tail is None else [s + t for s, t in zip(tail, new)]
    packed = pack_sums(accs[:8], 0) + pack_sums(accs[8:], 8)

    first, last = take_halo(ITERS, copies, -1.0)
    for a, extra in ((0, first), (P_SIZE - 1, last)):
        for p in range(PAIRS):
            v = tile(bas.at[ITERS], a, p) + jnp.where(edge, 0.0, extra[p] * powers[ITERS])
            put(bas.at[ITERS], a, p, v)
            vecs = [tile(bas.at[k], a, p) for k in range(ITERS)] + [v]
            tail = [s + u * v for s, u in zip(tail, vecs)]
    start_reduce(1, packed + pack_sums(tail, 16))
    sums = end_reduce(1)

    gram = {}
    for k, (i, j) in enumerate(pairs):
        gram[i, j] = sums(k) * (1.0 / total)
    for i in range(VECS):
        gram[i, ITERS] = sums(16 + i) * (1.0 / total)

    def times_gram(u, rows):
        return [
            dot((gram[min(i, r), max(i, r)], u[i]) for i in range(len(u))) for r in range(rows)
        ]

    hess = jnp.zeros((8, 128), jnp.float32)
    combos = [[1.0 / jnp.sqrt(gram[0, 0] + FLOOR)]]
    for j in range(ITERS):
        c = combos[j]
        u = [theta * c[0]]
        for i in range(1, j + 1):
            u.append(spread * c[i - 1] + theta * c[i])
        u.append(spread * c[j])
        g = times_gram(u, j + 1)
        rest = list(u)
        for i in range(j + 1):
            h = dot(zip(combos[i], g))
            hess = jnp.where((sub == i) & (lane == j), h, hess)
            for k in range(i + 1):
                rest[k] = rest[k] - h * combos[i][k]
        square = dot(zip(rest, times_gram(rest, j + 2)))
        beta = jnp.sqrt(jnp.maximum(square, 0.0) + FLOOR)
        hess = jnp.where((sub == j + 1) & (lane == j), beta, hess)
        post = 1.0 / beta
        combos.append([r * post for r in rest])

    for a, p in tiles():
        vecs = [tile(bas.at[k], a, p) for k in range(VECS)]
        for j in reversed(range(VECS)):
            put(bas.at[j], a, p, dot(zip(combos[j], vecs)))
    hess_out[...] = hess[0:VECS, 0:ITERS]

    for copy in started + narrow_copies + wide_copies:
        copy.wait_send()
    for slot in range(2):
        block = rrecv.at[slot, pl.ds(0, n - 1)]
        pltpu.make_async_copy(block, block, rs_sem.at[slot]).wait()


def store(hess, basis, hess_out, basis_out, sem):
    copies = [
        pltpu.make_async_copy(basis, basis_out, sem.at[0]),
        pltpu.make_async_copy(hess, hess_out, sem.at[1]),
    ]
    for copy in copies:
        copy.start()
    for copy in copies:
        copy.wait()


def body(nx, ny, source, initial, reaction, stiffness, line_op, face_deriv, wall_flags):
    nodes, ex, ey = source.shape
    n = nx * ny
    rows = nodes * ex
    flat = (rows, ey)
    blocks = len(block_offsets(nx))
    total = float(nodes * ex * nx * ey * ny)
    vmem = pl.BlockSpec(memory_space=pltpu.VMEM)
    hbm = pl.BlockSpec(memory_space=pl.ANY)
    smem = pl.BlockSpec(memory_space=pltpu.SMEM)

    def array(*lead):
        return pltpu.VMEM(lead + (8, 128), jnp.float32)

    dma = pltpu.SemaphoreType.DMA
    hess, basis = pl.pallas_call(
        functools.partial(kernel, nx, ny, total),
        out_shape=(
            pltpu.VMEM((VECS, ITERS), jnp.float32),
            pltpu.VMEM((VECS,) + flat, jnp.float32),
        ),
        in_specs=[smem, smem, hbm, hbm, hbm, vmem, vmem],
        out_specs=(vmem, vmem),
        scratch_shapes=[
            array(2 * PAIRS * PAIRS),
            array(2 * PAIRS),
            array(2 * PAIRS),
            array(2),
            array(4),
            pltpu.VMEM(flat, jnp.float32),
            pltpu.VMEM(flat, jnp.float32),
            pltpu.VMEM(flat, jnp.float32),
            array(blocks, WIDE),
            array(NARROW),
            array(NARROW),
            array(blocks, NARROW),
            array(blocks, NARROW),
            array(2, blocks * P_SIZE),
            array(2, blocks * P_SIZE),
            array(2, blocks * P_SIZE),
            array(2, blocks * 4),
            array(2, blocks * P_SIZE),
            array(2, blocks * P_SIZE),
            array(VECS, P_SIZE),
            dma((3,)),
            array(VECS, 2),
            array(VECS, 2),
            pltpu.VMEM((2, 1, 128), jnp.float32),
            pltpu.VMEM((2, n, 128), jnp.float32),
            dma((VECS, 2)),
            dma((VECS, 2)),
            dma((blocks,)),
            dma((blocks,)),
            dma((2, blocks)),
            dma((2, blocks)),
            dma((2,)),
            dma((2,)),
        ],
        compiler_params=pltpu.CompilerParams(collective_id=0, has_side_effects=True),
    )(
        line_op, face_deriv, source.reshape(flat), initial.reshape(flat), reaction.reshape(flat),
        stiffness, wall_flags,
    )
    hess = pltpu.with_memory_space_constraint(hess, pltpu.VMEM)
    basis = pltpu.with_memory_space_constraint(basis, pltpu.VMEM)
    hess, basis = pl.pallas_call(
        store,
        out_shape=(
            jax.ShapeDtypeStruct(hess.shape, jnp.float32),
            jax.ShapeDtypeStruct(basis.shape, jnp.float32),
        ),
        in_specs=[hbm, hbm],
        out_specs=(hbm, hbm),
        scratch_shapes=[pltpu.SemaphoreType.DMA((2,))],
    )(hess, basis)
    return hess, basis.reshape((VECS, nodes, ex, ey))


def solution(mesh):
    return jax.shard_map(
        functools.partial(body, mesh.shape["gx"], mesh.shape["gy"]),
        mesh=mesh,
        in_specs=(
            P(None, "gx", "gy"),
            P(None, "gx", "gy"),
            P(None, "gx", "gy"),
            P("gx", "gy"),
            P(),
            P(),
            P(None, "gx", "gy"),
        ),
        out_specs=(P(), P(None, None, "gx", "gy")),
        check_vma=False,
    )
```

```python
import functools

import jax
import jax.numpy as jnp
from jax import lax
from jax.experimental import pallas as pl
from jax.experimental.pallas import tpu as pltpu
from jax.sharding import PartitionSpec as P

P_SIZE = 8
ITERS = 5
VECS = ITERS + 1
TAU = 2.0
FLOOR = 0.1
PAIRS = P_SIZE // 2
SLOT = 32
GHOST = 8
WIDE = 2 * P_SIZE + 4
NARROW = 2 * 2 + 1
MESH = pl.DeviceIdType.MESH


def block_offsets(nx):
    near = min(nx, 5)
    return list(range(-((near - 1) // 2), near // 2 + 1))


def wrapped(o, nx):
    for same in (o, o - nx, o + nx):
        if same in block_offsets(nx):
            return same
    return None


def kernel(
    nx, ny, total,
    line, deriv, src_any, ini_any, rea_any, stf, wal,
    hess_out, bas,
    coef, gcoef, scoef, sgcoef, small, src, ini, rea,
    wide, low_send, high_send, south_in, north_in,
    page_rea, page_small, page_a, page_b, patch,
    in_sem, hsend, hrecv, ysend, yrecv, rsend, rrecv,
    hs_sem, hr_sem, ys_sem, yr_sem, ws_sem, wr_sem, ns_sem, nr_sem, rs_sem, rr_sem,
):
    n = nx * ny
    offs = block_offsets(nx)
    near = [o for o in offs if abs(o) <= 1]
    here = offs.index(0)
    gx, gy = lax.axis_index("gx"), lax.axis_index("gy")
    me = gx * ny + gy

    side = gy // (ny // 2)
    offsets = sorted(range(1, nx), key=lambda d: abs(2 * d - nx))

    def for_peers(act):
        def column(k, own_column):
            across = side * k + (1 - side) * (ny - 1 - k)
            for d in offsets:
                act((lax.rem(gx + d, nx), across))
            if own_column:
                skip = jnp.where(k >= (side * gy + (1 - side) * (ny - 1 - gy)), 1, 0)
                act((gx, across + (2 * side - 1) * skip))

        if n <= 64:
            for k in range(ny - 1):
                column(k, True)
        else:
            lax.fori_loop(0, ny - 1, lambda k, c: (column(k, True), c)[1], 0)
        column(ny - 1, False)

    def at(dx, dy):
        return (lax.rem(gx + dx + nx, nx), lax.rem(gy + dy + ny, ny))

    barrier = pltpu.get_barrier_semaphore()

    def greet(device):
        pl.semaphore_signal(barrier, inc=1, device_id=device, device_id_type=MESH)

    loads = [
        pltpu.make_async_copy(given, held, in_sem.at[k])
        for k, (given, held) in enumerate(((ini_any, ini), (src_any, src), (rea_any, rea)))
    ]
    for load in loads:
        load.start()
    for_peers(greet)

    sub = lax.broadcasted_iota(jnp.int32, (8, 128), 0)
    lane = lax.broadcasted_iota(jnp.int32, (8, 128), 1)
    low = sub < 4
    xpos = sub % 4
    slot_of = lane // SLOT
    in_slot = lane % SLOT
    south_half = in_slot < SLOT // 2

    def srl(v, s):
        s = s % 8
        return v if s == 0 else pltpu.roll(v, s, 0)

    def lrl(v, s):
        s = s % 128
        return v if s == 0 else pltpu.roll(v, s, 1)

    def halves(a, b):
        return jnp.where(low, a, b)

    def by_slot(parts):
        out = parts[0]
        for p in range(1, PAIRS):
            out = jnp.where(slot_of == p, parts[p], out)
        return out

    def dot(pairs):
        out = None
        for c, v in pairs:
            out = c * v if out is None else out + c * v
        return out

    mix = {}
    for p in range(PAIRS):
        for r in range(PAIRS):
            mix[p, r, 0] = halves(line[2 * p, 2 * r], line[2 * p + 1, 2 * r + 1])
            mix[p, r, 1] = halves(line[2 * p, 2 * r + 1], line[2 * p + 1, 2 * r])
            for k in range(2):
                coef[(p * PAIRS + r) * 2 + k] = mix[p, r, k]
    glow = [0.5 * deriv[c] + (TAU if c == 0 else 0.0) for c in range(P_SIZE)]
    gupp = [
        0.5 * deriv[P_SIZE - 1 - c] + (TAU if c == P_SIZE - 1 else 0.0) for c in range(P_SIZE)
    ]
    lows = [halves(glow[2 * p], glow[2 * p + 1]) for p in range(PAIRS)]
    upps = [halves(gupp[2 * p], gupp[2 * p + 1]) for p in range(PAIRS)]
    for p in range(PAIRS):
        gcoef[p] = lows[p]
        gcoef[PAIRS + p] = upps[p]
    small[0, 0:4] = stf[...]
    small[0, 4:8] = stf[...]
    opened = [1.0 - wal[f].astype(jnp.float32) for f in range(4)]
    for slot, (first, second) in enumerate(((0, 0), (1, 1), (2, 3))):
        small[slot + 1, 0:4] = opened[first]
        small[slot + 1, 4:8] = opened[second]
    trace = line[0, 0]
    for c in range(1, P_SIZE):
        trace = trace + line[c, c]
    shift = 3.0 + 0.25 * trace

    def tile(ref, a, p):
        return ref[pl.ds((a * PAIRS + p) * 8, 8), :]

    def put(ref, a, p, value):
        ref[pl.ds((a * PAIRS + p) * 8, 8), :] = value

    def tiles():
        return [(a, p) for a in range(P_SIZE) for p in range(PAIRS)]

    def xfaces(get):
        fw, fe = [], []
        for p in range(PAIRS):
            vs = [get(c, p) for c in range(P_SIZE)]
            fw.append(dot(zip(glow, vs)))
            fe.append(dot(zip(gupp, vs)))
        return fw, fe

    def halo_copy(slot, way, device):
        return pltpu.make_async_remote_copy(
            src_ref=hsend.at[slot, way],
            dst_ref=hrecv.at[slot, way],
            send_sem=hs_sem.at[slot, way],
            recv_sem=hr_sem.at[slot, way],
            device_id=device,
            device_id_type=MESH,
        )

    def send_halo(slot, faces, ready=lambda: None):
        fw, fe = faces
        cw, ce = fw[0], srl(fe[0], -3)
        for p in range(1, PAIRS):
            cw = jnp.where(xpos == p, srl(fw[p], p), cw)
            ce = jnp.where(xpos == p, srl(fe[p], p - 3), ce)
        hsend[slot, 0] = cw
        hsend[slot, 1] = ce
        ready()
        copies = [halo_copy(slot, 0, at(-1, 0)), halo_copy(slot, 1, at(1, 0))]
        for copy in copies:
            copy.start()
        return copies

    def take_halo(slot, copies, sign):
        for copy in copies:
            copy.wait_recv()
        cw, ce = hrecv[slot, 0], hrecv[slot, 1]
        open_w, open_e = small[1] * sign, small[2] * sign
        first = [open_w * jnp.where(xpos == 0, srl(ce, -p), 0.0) for p in range(PAIRS)]
        last = [open_e * jnp.where(xpos == 3, srl(cw, 3 - p), 0.0) for p in range(PAIRS)]
        return first, last

    edge_lane = lane == jnp.where(low, 0, 127)

    def yfaces(get):
        own, across = [], []
        for a in range(P_SIZE):
            vs = [get(a, p) for p in range(PAIRS)]
            s = dot((gcoef[p], vs[p]) for p in range(PAIRS))
            t = dot((gcoef[PAIRS + p], vs[p]) for p in range(PAIRS))
            u = halves(s, t) + srl(halves(t, s), 4)
            q = srl(u, 4)
            own.append(u)
            across.append(halves(lrl(q, 1), lrl(q, 127)))
        return own, across

    def y_copy(target, device):
        return pltpu.make_async_remote_copy(
            src_ref=ysend,
            dst_ref=yrecv.at[target],
            send_sem=ys_sem.at[target],
            recv_sem=yr_sem.at[target],
            device_id=device,
            device_id_type=MESH,
        )

    def y_copies():
        return [y_copy(0, at(0, 1)), y_copy(1, at(0, -1))]

    def send_yfaces(across):
        packed = across[0]
        for a in range(1, P_SIZE):
            mask = lane == jnp.where(low, a, a - 1)
            packed = jnp.where(mask, lrl(across[a], a), packed)
        ysend[...] = packed
        for copy in y_copies():
            copy.start()

    def operate(get, faces, given, emit):
        fw, fe = faces
        own, across = given or yfaces(get)
        stiff, open_w, open_e, open_y = small[0], small[1], small[2], small[3]
        sides = {}
        for p in range(PAIRS):
            nb_e = jnp.where(xpos == 3, 0.0, srl(fw[p], 7))
            nb_w = jnp.where(xpos == 0, 0.0, srl(fe[p], 1))
            sides[0, p] = fw[p] - open_w * nb_w
            sides[P_SIZE - 1, p] = fe[p] - open_e * nb_e
        for a in range(P_SIZE):
            vs = [get(a, p) for p in range(PAIRS)]
            ss = [srl(v, 4) for v in vs]
            beside = jnp.where(edge_lane, 0.0, across[a]) if given else across[a]
            term = own[a] - open_y * beside
            for p in range(PAIRS):
                acc = None
                for r in range(PAIRS):
                    k = (p * PAIRS + r) * 2
                    part = coef[k] * vs[r] + coef[k + 1] * ss[r]
                    acc = part if acc is None else acc + part
                other = dot((line[a, c], get(c, p)) for c in range(P_SIZE))
                react = tile(rea, a, p) if given else tile(rea, a, p) - shift
                value = react * vs[p] + stiff * (acc + other)
                if p == 0:
                    value = value + jnp.where(low, term, 0.0)
                if p == PAIRS - 1:
                    value = value + jnp.where(low, 0.0, term)
                if (a, p) in sides:
                    value = value + sides[a, p]
                emit(a, p, value)

    def gather_rows(accs):
        zero = jnp.zeros((8, 128), jnp.float32)
        level = list(accs) + [zero] * (8 - len(accs))
        for step in (1, 2, 4):
            keep = (sub // step) % 2 == 0
            level = [
                jnp.where(keep, level[i], level[i + 1])
                + srl(jnp.where(keep, level[i + 1], level[i]), step)
                for i in range(0, len(level), 2)
            ]
        return level[0]

    def fold(v):
        for step in (4, 2, 1):
            v = v + srl(v, step)
        return v

    def row_copy(slot, device):
        return pltpu.make_async_remote_copy(
            src_ref=rsend.at[slot],
            dst_ref=rrecv.at[slot, pl.ds(me, 1)],
            send_sem=rs_sem.at[slot],
            recv_sem=rr_sem.at[slot],
            device_id=device,
            device_id_type=MESH,
        )

    def pack_sums(accs, start):
        sums = jnp.sum(gather_rows(accs), axis=1, keepdims=True)
        return jnp.where(lane == sub + start, sums, 0.0)

    def start_reduce(slot, packed):
        row = fold(packed)[0:1]
        rsend[slot] = row
        rrecv[slot, pl.ds(me, 1)] = row
        for_peers(lambda device: row_copy(slot, device).start())

    def end_reduce(slot):
        block = rrecv.at[slot, pl.ds(0, n - 1)]
        pltpu.make_async_copy(block, block, rr_sem.at[slot]).wait()
        value = rrecv[slot, 0:8]
        for g in range(1, n // 8):
            value = value + rrecv[slot, 8 * g:8 * g + 8]
        value = fold(value)
        return lambda k: jnp.broadcast_to(value[:, k:k + 1], (8, 128))

    def narrow_copy(late, o, dy):
        sent, held = (low_send, north_in) if dy < 0 else (high_send, south_in)
        rows = pl.ds(0, 2) if late else pl.ds(2, 3)
        j = near.index(wrapped(-o, nx))
        sems = (1 if late else 0, 0 if dy < 0 else 1, j)
        return pltpu.make_async_remote_copy(
            src_ref=sent.at[rows],
            dst_ref=held.at[j, rows],
            send_sem=ns_sem.at[sems],
            recv_sem=nr_sem.at[sems],
            device_id=at(o, dy),
            device_id_type=MESH,
        )

    def wide_copy(late, o):
        rows = pl.ds(0, P_SIZE) if late else pl.ds(P_SIZE, P_SIZE + 4)
        j = offs.index(wrapped(-o, nx))
        sems = (1 if late else 0, j)
        return pltpu.make_async_remote_copy(
            src_ref=wide.at[here, rows],
            dst_ref=wide.at[j, rows],
            send_sem=ws_sem.at[sems],
            recv_sem=wr_sem.at[sems],
            device_id=at(o, 0),
            device_id_type=MESH,
        )

    def strip_copies(late):
        return [narrow_copy(late, o, dy) for dy in (-1, 1) for o in near] + [
            wide_copy(late, o) for o in sorted(offs, key=abs) if o
        ]

    def gathered(parts):
        return by_slot([lrl(parts[p], 16 + SLOT * p) for p in range(PAIRS)])

    def pack_narrow(items, index):
        for ref, start in ((low_send, 16), (high_send, 8)):
            out = None
            for i, v in enumerate(items):
                moved = lrl(v, GHOST * i - start)
                out = moved if out is None else jnp.where(in_slot // GHOST == i, moved, out)
            ref[index] = out

    def pack_field(ref, wide_at, narrow_at):
        for quad in range(2):
            items = []
            for a in range(4 * quad, 4 * quad + 4):
                v = gathered([tile(ref, a, p) for p in range(PAIRS)])
                wide[here, wide_at + a] = v
                items.append(v)
            pack_narrow(items, narrow_at + quad)

    def pack_small():
        items = []
        for f in range(4):
            v = gathered([small[f]] * PAIRS)
            wide[here, 2 * P_SIZE + f] = v
            items.append(v)
        pack_narrow(items, 4)

    def finish_first():
        for copy in y_copies():
            copy.wait_recv()
        cy = halves(yrecv[0], yrecv[1])
        first = bas.at[0]
        for a in range(P_SIZE):
            term = small[3] * jnp.where(edge_lane, lrl(cy, -a), 0.0)
            put(first, a, 0, tile(first, a, 0) + jnp.where(low, term, 0.0))
            last = PAIRS - 1
            put(first, a, last, tile(first, a, last) + jnp.where(low, 0.0, term))
        pack_field(first, 0, 0)
        for copy in strip_copies(True):
            copy.start()

    for d in range(PAIRS):
        for k in range(2):
            scoef[2 * d + k] = by_slot([mix[(r + d) % PAIRS, r, k] for r in range(PAIRS)])
    sgcoef[0] = by_slot(lows)
    sgcoef[1] = by_slot(upps)
    y_mask = (low & (slot_of == 0)) | (~low & (slot_of == PAIRS - 1))

    def unpack_pages():
        def merge(seam, o, wide_at, narrow_at, i):
            wide_part = wide[offs.index(o), wide_at]
            if o not in near:
                return wide_part
            narrow_part = (south_in, north_in)[seam][near.index(o), narrow_at]
            if seam == 0:
                return jnp.where(south_half, lrl(narrow_part, GHOST - GHOST * i), wide_part)
            return jnp.where(south_half, wide_part, lrl(narrow_part, 16 - GHOST * i))

        for seam in range(2):
            for j, o in enumerate(offs):
                for a in range(P_SIZE):
                    page_a[seam, j * P_SIZE + a] = merge(seam, o, a, a // 4, a % 4)
                    if o in near:
                        page_rea[seam, j * P_SIZE + a] = (
                            merge(seam, o, P_SIZE + a, 2 + a // 4, a % 4) - shift
                        )
                if o in near:
                    for f in range(4):
                        page_small[seam, j * 4 + f] = merge(seam, o, 2 * P_SIZE + f, 4, f)

    def page_level(level):
        given, out = (page_a, page_b) if level % 2 else (page_b, page_a)
        targets = near if level < ITERS else [0]

        def known(o):
            o = wrapped(o, nx)
            return o is not None and (level == 1 or o in near)

        for seam in range(2):
            def face(weights, o):
                j = offs.index(wrapped(o, nx)) * P_SIZE
                return dot((weights[a], given[seam, j + a]) for a in range(P_SIZE))

            for o in targets:
                j = offs.index(o)
                stiff, open_w, open_e, open_y = [page_small[seam, j * 4 + f] for f in range(4)]
                fw, fe = face(glow, o), face(gupp, o)
                nb_e, nb_w = srl(fw, 7), srl(fe, 1)
                if known(o + 1):
                    nb_e = jnp.where(xpos == 3, srl(face(glow, o + 1), 3), nb_e)
                if known(o - 1):
                    nb_w = jnp.where(xpos == 0, srl(face(gupp, o - 1), 5), nb_w)
                sides = {0: fw - open_w * nb_w, P_SIZE - 1: fe - open_e * nb_e}
                vs = [given[seam, j * P_SIZE + a] for a in range(P_SIZE)]
                for a in range(P_SIZE):
                    v = vs[a]
                    ss = srl(v, 4)
                    acc = scoef[0] * v + scoef[1] * ss
                    for d in range(1, PAIRS):
                        acc = acc + lrl(scoef[2 * d] * v + scoef[2 * d + 1] * ss, SLOT * d)
                    s, t = sgcoef[0] * v, sgcoef[1] * v
                    own = halves(s, t) + srl(halves(t, s), 4)
                    own = (own + lrl(own, 64)) + (lrl(own, 32) + lrl(own, 96))
                    q = srl(own, 4)
                    term = own - open_y * halves(lrl(q, 1), lrl(q, 127))
                    other = dot(zip([line[a, c] for c in range(P_SIZE)], vs))
                    value = page_rea[seam, j * P_SIZE + a] * v + stiff * (acc + other)
                    value = value + jnp.where(y_mask, term, 0.0)
                    if a in sides:
                        value = value + sides[a]
                    out[seam, j * P_SIZE + a] = value
        for a in range(P_SIZE):
            k = here * P_SIZE + a
            patch[level, a] = jnp.where(south_half, out[1, k], out[0, k])

    edge = (lane < VECS) | (lane >= 128 - VECS)

    def patched(level, a, p, v):
        if level == 0:
            return v
        return jnp.where(edge, lrl(patch[level, a], 112 - SLOT * p), v)

    started = []

    loads[0].wait()
    get = functools.partial(tile, ini)
    faces = xfaces(get)
    copies = send_halo(0, faces, lambda: pl.semaphore_wait(barrier, n - 1))
    started += copies
    given = yfaces(get)
    send_yfaces(given[1])
    loads[1].wait()
    loads[2].wait()
    operate(get, faces, given, lambda a, p, v: put(bas.at[0], a, p, tile(src, a, p) - v))
    pack_field(rea, P_SIZE, 2)
    pack_small()
    for copy in strip_copies(False):
        copy.start()

    late = gy == ny - 1
    for level in range(ITERS):
        now = bas.at[level]
        get = functools.partial(tile, now)
        fw, fe = xfaces(get)
        first, last = take_halo(level, copies, 1.0 if level == 0 else -1.0)
        fw = [fw[p] + glow[0] * first[p] + glow[P_SIZE - 1] * last[p] for p in range(PAIRS)]
        fe = [fe[p] + gupp[0] * first[p] + gupp[P_SIZE - 1] * last[p] for p in range(PAIRS)]
        copies = send_halo(level + 1, (fw, fe))
        started += copies
        for p in range(PAIRS):
            put(now, 0, p, get(0, p) + first[p])
            put(now, P_SIZE - 1, p, get(P_SIZE - 1, p) + last[p])
        operate(get, (fw, fe), None, functools.partial(put, bas.at[level + 1]))
        if level == 0:
            pl.when(jnp.logical_not(late))(finish_first)
        if level == 1:
            pl.when(late)(finish_first)
            accs = [None] * 3
            for a, p in tiles():
                u, v = tile(bas.at[0], a, p), tile(bas.at[1], a, p)
                new = [u * u, u * v, v * v]
                accs = new if accs[0] is None else [s + t for s, t in zip(accs, new)]
            start_reduce(0, pack_sums(accs, 0))
        if level == 3:
            for copy in strip_copies(False) + strip_copies(True):
                copy.wait_recv()
            unpack_pages()
            page_level(1)
            page_level(2)
        if level == 4:
            for k in range(3, VECS):
                page_level(k)

    sums = end_reduce(0)
    size = jnp.maximum(sums(0), 1e-30)
    mean = sums(1) / size
    spread = jnp.sqrt(jnp.maximum(sums(2) / size - mean * mean, 0.0)) + 0.1
    inv = 1.0 / spread
    ratio = mean * inv
    theta = shift + mean
    powers = [None, inv]
    for k in range(2, VECS):
        powers.append(powers[k - 1] * inv)

    pairs = [(i, j) for j in range(ITERS) for i in range(j + 1)]
    accs, tail = None, None
    for a, p in tiles():
        lev = []
        for k in range(VECS):
            v = patched(k, a, p, tile(bas.at[k], a, p))
            lev.append(v if k == 0 else v * powers[k])
        vecs = [lev[0]]
        for k in range(1, VECS):
            lev = [lev[i + 1] - ratio * lev[i] for i in range(len(lev) - 1)]
            vecs.append(lev[0])
        for k in range(1, VECS):
            put(bas.at[k], a, p, vecs[k])
        put(bas.at[0], a, p, vecs[0])
        new = [vecs[i] * vecs[j] for i, j in pairs]
        accs = new if accs is None else [s + t for s, t in zip(accs, new)]
        if 0 < a < P_SIZE - 1:
            new = [v * vecs[ITERS] for v in vecs]
            tail = new if tail is None else [s + t for s, t in zip(tail, new)]
    packed = pack_sums(accs[:8], 0) + pack_sums(accs[8:], 8)

    first, last = take_halo(ITERS, copies, -1.0)
    for a, extra in ((0, first), (P_SIZE - 1, last)):
        for p in range(PAIRS):
            v = tile(bas.at[ITERS], a, p) + jnp.where(edge, 0.0, extra[p] * powers[ITERS])
            put(bas.at[ITERS], a, p, v)
            vecs = [tile(bas.at[k], a, p) for k in range(ITERS)] + [v]
            tail = [s + u * v for s, u in zip(tail, vecs)]
    start_reduce(1, packed + pack_sums(tail, 16))
    sums = end_reduce(1)

    gram = {}
    for k, (i, j) in enumerate(pairs):
        gram[i, j] = sums(k) * (1.0 / total)
    for i in range(VECS):
        gram[i, ITERS] = sums(16 + i) * (1.0 / total)

    def times_gram(u, rows):
        return [
            dot((gram[min(i, r), max(i, r)], u[i]) for i in range(len(u))) for r in range(rows)
        ]

    hess = jnp.zeros((8, 128), jnp.float32)
    combos = [[1.0 / jnp.sqrt(gram[0, 0] + FLOOR)]]
    for j in range(ITERS):
        c = combos[j]
        u = [theta * c[0]]
        for i in range(1, j + 1):
            u.append(spread * c[i - 1] + theta * c[i])
        u.append(spread * c[j])
        g = times_gram(u, j + 1)
        rest = list(u)
        for i in range(j + 1):
            h = dot(zip(combos[i], g))
            hess = jnp.where((sub == i) & (lane == j), h, hess)
            for k in range(i + 1):
                rest[k] = rest[k] - h * combos[i][k]
        square = dot(zip(rest, times_gram(rest, j + 2)))
        beta = jnp.sqrt(jnp.maximum(square, 0.0) + FLOOR)
        hess = jnp.where((sub == j + 1) & (lane == j), beta, hess)
        post = 1.0 / beta
        combos.append([r * post for r in rest])

    for a, p in tiles():
        vecs = [tile(bas.at[k], a, p) for k in range(VECS)]
        for j in reversed(range(VECS)):
            put(bas.at[j], a, p, dot(zip(combos[j], vecs)))
    hess_out[...] = hess[0:VECS, 0:ITERS]

    for copy in started + y_copies() + strip_copies(False) + strip_copies(True):
        copy.wait_send()
    for slot in range(2):
        block = rrecv.at[slot, pl.ds(0, n - 1)]
        pltpu.make_async_copy(block, block, rs_sem.at[slot]).wait()


def store(hess, basis, hess_out, basis_out, sem):
    copies = [
        pltpu.make_async_copy(basis, basis_out, sem.at[0]),
        pltpu.make_async_copy(hess, hess_out, sem.at[1]),
    ]
    for copy in copies:
        copy.start()
    for copy in copies:
        copy.wait()


def body(nx, ny, source, initial, reaction, stiffness, line_op, face_deriv, wall_flags):
    nodes, ex, ey = source.shape
    n = nx * ny
    rows = nodes * ex
    flat = (rows, ey)
    offs = block_offsets(nx)
    blocks = len(offs)
    near = len([o for o in offs if abs(o) <= 1])
    total = float(nodes * ex * nx * ey * ny)
    vmem = pl.BlockSpec(memory_space=pltpu.VMEM)
    hbm = pl.BlockSpec(memory_space=pl.ANY)
    smem = pl.BlockSpec(memory_space=pltpu.SMEM)

    def array(*lead):
        return pltpu.VMEM(lead + (8, 128), jnp.float32)

    dma = pltpu.SemaphoreType.DMA
    hess, basis = pl.pallas_call(
        functools.partial(kernel, nx, ny, total),
        out_shape=(
            pltpu.VMEM((VECS, ITERS), jnp.float32),
            pltpu.VMEM((VECS,) + flat, jnp.float32),
        ),
        in_specs=[smem, smem, hbm, hbm, hbm, vmem, vmem],
        out_specs=(vmem, vmem),
        scratch_shapes=[
            array(2 * PAIRS * PAIRS),
            array(2 * PAIRS),
            array(2 * PAIRS),
            array(2),
            array(4),
            pltpu.VMEM(flat, jnp.float32),
            pltpu.VMEM(flat, jnp.float32),
            pltpu.VMEM(flat, jnp.float32),
            array(blocks, WIDE),
            array(NARROW),
            array(NARROW),
            array(near, NARROW),
            array(near, NARROW),
            array(2, blocks * P_SIZE),
            array(2, blocks * 4),
            array(2, blocks * P_SIZE),
            array(2, blocks * P_SIZE),
            array(VECS, P_SIZE),
            dma((3,)),
            array(VECS, 2),
            array(VECS, 2),
            array(),
            array(2),
            pltpu.VMEM((2, 1, 128), jnp.float32),
            pltpu.VMEM((2, n, 128), jnp.float32),
            dma((VECS, 2)),
            dma((VECS, 2)),
            dma((2,)),
            dma((2,)),
            dma((2, blocks)),
            dma((2, blocks)),
            dma((2, 2, near)),
            dma((2, 2, near)),
            dma((2,)),
            dma((2,)),
        ],
        compiler_params=pltpu.CompilerParams(collective_id=0, has_side_effects=True),
    )(
        line_op, face_deriv, source.reshape(flat), initial.reshape(flat), reaction.reshape(flat),
        stiffness, wall_flags,
    )
    hess = pltpu.with_memory_space_constraint(hess, pltpu.VMEM)
    basis = pltpu.with_memory_space_constraint(basis, pltpu.VMEM)
    hess, basis = pl.pallas_call(
        store,
        out_shape=(
            jax.ShapeDtypeStruct(hess.shape, jnp.float32),
            jax.ShapeDtypeStruct(basis.shape, jnp.float32),
        ),
        in_specs=[hbm, hbm],
        out_specs=(hbm, hbm),
        scratch_shapes=[pltpu.SemaphoreType.DMA((2,))],
    )(hess, basis)
    return hess, basis.reshape((VECS, nodes, ex, ey))


def solution(mesh):
    return jax.shard_map(
        functools.partial(body, mesh.shape["gx"], mesh.shape["gy"]),
        mesh=mesh,
        in_specs=(
            P(None, "gx", "gy"),
            P(None, "gx", "gy"),
            P(None, "gx", "gy"),
            P("gx", "gy"),
            P(),
            P(),
            P(None, "gx", "gy"),
        ),
        out_specs=(P(), P(None, None, "gx", "gy")),
        check_vma=False,
    )
```

```python
import functools

import jax
import jax.numpy as jnp
from jax import lax
from jax.experimental import pallas as pl
from jax.experimental.pallas import tpu as pltpu
from jax.sharding import PartitionSpec as P

P_SIZE = 8
ITERS = 5
VECS = ITERS + 1
TAU = 2.0
FLOOR = 0.1
PAIRS = P_SIZE // 2
SLOT = 16
GHOSTS = ITERS
OWNED = SLOT - GHOSTS
WIDE = 2 * P_SIZE + 1
NARROW = P_SIZE + 1
MESH = pl.DeviceIdType.MESH


def kernel(
    nx, ny, total,
    line, deriv, src_any, ini_any, rea_any, stf, wal,
    hess_out, bas,
    coef, gcoef, small, src, ini, rea,
    wide, narrow, narrow_in, far_send, far_in,
    page_rea, page_small, page_a, page_b, patch,
    in_sem, hsend, hrecv, ysend, yrecv, rsend, rrecv,
    hs_sem, hr_sem, ys_sem, yr_sem, ws_sem, wr_sem, ns_sem, nr_sem,
    fs_sem, fr_sem, rs_sem, rr_sem,
):
    n = nx * ny
    gx, gy = lax.axis_index("gx"), lax.axis_index("gy")
    me = gx * ny + gy

    side = gy // (ny // 2)
    offsets = sorted(range(1, nx), key=lambda d: abs(2 * d - nx))

    def for_peers(act):
        def column(k, own_column):
            across = side * k + (1 - side) * (ny - 1 - k)
            for d in offsets:
                act((lax.rem(gx + d, nx), across))
            if own_column:
                skip = jnp.where(k >= (side * gy + (1 - side) * (ny - 1 - gy)), 1, 0)
                act((gx, across + (2 * side - 1) * skip))

        if n <= 64:
            for k in range(ny - 1):
                column(k, True)
        else:
            lax.fori_loop(0, ny - 1, lambda k, c: (column(k, True), c)[1], 0)
        column(ny - 1, False)

    def at(dx, dy):
        return (lax.rem(gx + dx + nx, nx), lax.rem(gy + dy + ny, ny))

    barrier = pltpu.get_barrier_semaphore()

    def greet(device):
        pl.semaphore_signal(barrier, inc=1, device_id=device, device_id_type=MESH)

    loads = [
        pltpu.make_async_copy(given, held, in_sem.at[k])
        for k, (given, held) in enumerate(((ini_any, ini), (src_any, src), (rea_any, rea)))
    ]
    for load in loads:
        load.start()
    for_peers(greet)

    sub = lax.broadcasted_iota(jnp.int32, (8, 128), 0)
    lane = lax.broadcasted_iota(jnp.int32, (8, 128), 1)
    low = sub < 4
    xpos = sub % 4
    def srl(v, s):
        s = s % 8
        return v if s == 0 else pltpu.roll(v, s, 0)

    def lrl(v, s):
        s = s % 128
        return v if s == 0 else pltpu.roll(v, s, 1)

    def halves(a, b):
        return jnp.where(low, a, b)

    def within(start, count):
        return (lane >= start) & (lane < start + count)

    def overlay(parts):
        out = None
        for mask, v in parts:
            out = v if out is None else jnp.where(mask, v, out)
        return out

    def dot(pairs):
        out = None
        for c, v in pairs:
            out = c * v if out is None else out + c * v
        return out

    for p in range(PAIRS):
        for r in range(PAIRS):
            k = (p * PAIRS + r) * 2
            coef[k] = halves(line[2 * p, 2 * r], line[2 * p + 1, 2 * r + 1])
            coef[k + 1] = halves(line[2 * p, 2 * r + 1], line[2 * p + 1, 2 * r])
    glow = [0.5 * deriv[c] + (TAU if c == 0 else 0.0) for c in range(P_SIZE)]
    gupp = [
        0.5 * deriv[P_SIZE - 1 - c] + (TAU if c == P_SIZE - 1 else 0.0) for c in range(P_SIZE)
    ]
    for p in range(PAIRS):
        gcoef[p] = halves(glow[2 * p], glow[2 * p + 1])
        gcoef[PAIRS + p] = halves(gupp[2 * p], gupp[2 * p + 1])
    small[0, 0:4] = stf[...]
    small[0, 4:8] = stf[...]
    opened = [1.0 - wal[f].astype(jnp.float32) for f in range(4)]
    for slot, (first, second) in enumerate(((0, 0), (1, 1), (2, 3))):
        small[slot + 1, 0:4] = opened[first]
        small[slot + 1, 4:8] = opened[second]
    trace = line[0, 0]
    for c in range(1, P_SIZE):
        trace = trace + line[c, c]
    shift = 3.0 + 0.25 * trace

    def tile(ref, a, p):
        return ref[pl.ds((a * PAIRS + p) * 8, 8), :]

    def put(ref, a, p, value):
        ref[pl.ds((a * PAIRS + p) * 8, 8), :] = value

    def tiles():
        return [(a, p) for a in range(P_SIZE) for p in range(PAIRS)]

    def xfaces(get):
        fw, fe = [], []
        for p in range(PAIRS):
            vs = [get(c, p) for c in range(P_SIZE)]
            fw.append(dot(zip(glow, vs)))
            fe.append(dot(zip(gupp, vs)))
        return fw, fe

    def halo_copy(slot, way, device):
        return pltpu.make_async_remote_copy(
            src_ref=hsend.at[slot, way],
            dst_ref=hrecv.at[slot, way],
            send_sem=hs_sem.at[slot, way],
            recv_sem=hr_sem.at[slot, way],
            device_id=device,
            device_id_type=MESH,
        )

    def pack_faces(faces):
        fw, fe = faces
        cw, ce = fw[0], srl(fe[0], -3)
        for p in range(1, PAIRS):
            cw = jnp.where(xpos == p, srl(fw[p], p), cw)
            ce = jnp.where(xpos == p, srl(fe[p], p - 3), ce)
        return cw, ce

    def send_halo(slot, faces, ready=lambda: None):
        cw, ce = pack_faces(faces)
        hsend[slot, 0] = cw
        hsend[slot, 1] = ce
        ready()
        copies = [halo_copy(slot, 0, at(-1, 0)), halo_copy(slot, 1, at(1, 0))]
        for copy in copies:
            copy.start()
        return copies

    def take_halo(slot, copies, sign):
        for copy in copies:
            copy.wait_recv()
        cw, ce = hrecv[slot, 0], hrecv[slot, 1]
        open_w, open_e = small[1] * sign, small[2] * sign
        first = [open_w * jnp.where(xpos == 0, srl(ce, -p), 0.0) for p in range(PAIRS)]
        last = [open_e * jnp.where(xpos == 3, srl(cw, 3 - p), 0.0) for p in range(PAIRS)]
        return first, last

    edge_lane = lane == jnp.where(low, 0, 127)

    def yfaces(get):
        own, across = [], []
        for a in range(P_SIZE):
            vs = [get(a, p) for p in range(PAIRS)]
            s = dot((gcoef[p], vs[p]) for p in range(PAIRS))
            t = dot((gcoef[PAIRS + p], vs[p]) for p in range(PAIRS))
            u = halves(s, t) + srl(halves(t, s), 4)
            q = srl(u, 4)
            own.append(u)
            across.append(halves(lrl(q, 1), lrl(q, 127)))
        return own, across

    def y_copy(target, device):
        return pltpu.make_async_remote_copy(
            src_ref=ysend,
            dst_ref=yrecv.at[target],
            send_sem=ys_sem.at[target],
            recv_sem=yr_sem.at[target],
            device_id=device,
            device_id_type=MESH,
        )

    def y_copies():
        return [y_copy(0, at(0, 1)), y_copy(1, at(0, -1))]

    def send_yfaces(across):
        packed = across[0]
        for a in range(1, P_SIZE):
            mask = lane == jnp.where(low, a, a - 1)
            packed = jnp.where(mask, lrl(across[a], a), packed)
        ysend[...] = packed
        for copy in y_copies():
            copy.start()

    def apply(get, react, fields, sides, own, across, emit):
        stiff, open_w, open_e, open_y = fields
        for a in range(P_SIZE):
            vs = [get(a, p) for p in range(PAIRS)]
            ss = [srl(v, 4) for v in vs]
            term = own[a] - open_y * across[a]
            for p in range(PAIRS):
                acc = None
                for r in range(PAIRS):
                    k = (p * PAIRS + r) * 2
                    part = coef[k] * vs[r] + coef[k + 1] * ss[r]
                    acc = part if acc is None else acc + part
                other = dot((line[a, c], get(c, p)) for c in range(P_SIZE))
                value = react(a, p) * vs[p] + stiff * (acc + other)
                if p == 0:
                    value = value + jnp.where(low, term, 0.0)
                if p == PAIRS - 1:
                    value = value + jnp.where(low, 0.0, term)
                if (a, p) in sides:
                    value = value + sides[a, p]
                emit(a, p, value)

    def operate(get, faces, given, emit):
        fw, fe = faces
        fields = [small[f] for f in range(4)]
        sides = {}
        for p in range(PAIRS):
            nb_e = jnp.where(xpos == 3, 0.0, srl(fw[p], 7))
            nb_w = jnp.where(xpos == 0, 0.0, srl(fe[p], 1))
            sides[0, p] = fw[p] - fields[1] * nb_w
            sides[P_SIZE - 1, p] = fe[p] - fields[2] * nb_e
        own, across = given or yfaces(get)
        if given:
            across = [jnp.where(edge_lane, 0.0, v) for v in across]
            react = functools.partial(tile, rea)
        else:
            react = lambda a, p: tile(rea, a, p) - shift
        apply(get, react, fields, sides, own, across, emit)

    def gather_rows(accs):
        zero = jnp.zeros((8, 128), jnp.float32)
        level = list(accs) + [zero] * (8 - len(accs))
        for step in (1, 2, 4):
            keep = (sub // step) % 2 == 0
            level = [
                jnp.where(keep, level[i], level[i + 1])
                + srl(jnp.where(keep, level[i + 1], level[i]), step)
                for i in range(0, len(level), 2)
            ]
        return level[0]

    def fold(v):
        for step in (4, 2, 1):
            v = v + srl(v, step)
        return v

    def row_copy(slot, device):
        return pltpu.make_async_remote_copy(
            src_ref=rsend.at[slot],
            dst_ref=rrecv.at[slot, pl.ds(me, 1)],
            send_sem=rs_sem.at[slot],
            recv_sem=rr_sem.at[slot],
            device_id=device,
            device_id_type=MESH,
        )

    def pack_sums(accs, start):
        sums = jnp.sum(gather_rows(accs), axis=1, keepdims=True)
        return jnp.where(lane == sub + start, sums, 0.0)

    def start_reduce(slot, packed):
        row = fold(packed)[0:1]
        rsend[slot] = row
        rrecv[slot, pl.ds(me, 1)] = row
        for_peers(lambda device: row_copy(slot, device).start())

    def end_reduce(slot):
        block = rrecv.at[slot, pl.ds(0, n - 1)]
        pltpu.make_async_copy(block, block, rr_sem.at[slot]).wait()
        value = rrecv[slot, 0:8]
        for g in range(1, n // 8):
            value = value + rrecv[slot, 8 * g:8 * g + 8]
        value = fold(value)
        return lambda k: jnp.broadcast_to(value[:, k:k + 1], (8, 128))

    near = (-1, 0, 1)

    def narrow_copy(late, o, dy):
        rows = pl.ds(0, PAIRS) if late else pl.ds(PAIRS, PAIRS + 1)
        side, j = (0 if dy > 0 else 1), near.index(-o)
        sems = (1 if late else 0, side, j)
        return pltpu.make_async_remote_copy(
            src_ref=narrow.at[rows],
            dst_ref=narrow_in.at[side, j, rows],
            send_sem=ns_sem.at[sems],
            recv_sem=nr_sem.at[sems],
            device_id=at(o, dy),
            device_id_type=MESH,
        )

    def wide_copy(late, o):
        rows = pl.ds(0, P_SIZE) if late else pl.ds(P_SIZE, P_SIZE + 1)
        j = near.index(-o)
        sems = (1 if late else 0, j)
        return pltpu.make_async_remote_copy(
            src_ref=wide.at[1, rows],
            dst_ref=wide.at[j, rows],
            send_sem=ws_sem.at[sems],
            recv_sem=wr_sem.at[sems],
            device_id=at(o, 0),
            device_id_type=MESH,
        )

    def far_copy(way, o):
        return pltpu.make_async_remote_copy(
            src_ref=far_send.at[way],
            dst_ref=far_in.at[way],
            send_sem=fs_sem.at[way],
            recv_sem=fr_sem.at[way],
            device_id=at(o, 0),
            device_id_type=MESH,
        )

    def strip_copies(late):
        copies = [narrow_copy(late, o, dy) for dy in (-1, 1) for o in near]
        copies += [wide_copy(late, o) for o in (-1, 1)]
        if late:
            copies += [far_copy(0, -2), far_copy(1, 2)]
        return copies

    def pack_wide(items, index):
        parts = []
        for p, v in enumerate(items):
            parts.append((within(32 * p, SLOT), lrl(v, 32 * p)))
            spot = (32 * p + 48) % 128
            parts.append((within(spot, SLOT), lrl(v, spot - (128 - OWNED))))
        wide[1, index] = overlay(parts)

    def pack_narrow(pairs, index):
        parts = []
        for i, items in enumerate(pairs):
            for p, v in enumerate(items):
                spot = SLOT * p + 8 * i
                parts.append((within(spot, 8), lrl(v, spot - (128 - GHOSTS))))
                parts.append((within(64 + spot, 8), lrl(v, 64 + spot)))
        narrow[index] = overlay(parts)

    def pack_field(ref, wide_at, narrow_at):
        rows = [[tile(ref, a, p) for p in range(PAIRS)] for a in range(P_SIZE)]
        for a in range(P_SIZE):
            pack_wide(rows[a], wide_at + a)
        for q in range(PAIRS):
            pack_narrow(rows[2 * q:2 * q + 2], narrow_at + q)

    def pack_small():
        items = [small[f] for f in range(4)]
        pack_wide(items, 2 * P_SIZE)
        pack_narrow([items], 2 * PAIRS)

    def finish_first():
        for copy in y_copies():
            copy.wait_recv()
        cy = halves(yrecv[0], yrecv[1])
        first = bas.at[0]
        for a in range(P_SIZE):
            term = small[3] * jnp.where(edge_lane, lrl(cy, -a), 0.0)
            put(first, a, 0, tile(first, a, 0) + jnp.where(low, term, 0.0))
            last = PAIRS - 1
            put(first, a, last, tile(first, a, last) + jnp.where(low, 0.0, term))
        cw, ce = pack_faces(xfaces(functools.partial(tile, first)))
        far_send[0] = cw
        far_send[1] = ce
        pack_field(first, 0, 0)
        for copy in strip_copies(True):
            copy.start()

    def unpack(wide_at, narrow_at, i, p):
        parts = []
        for j in range(3):
            mask = within(SLOT * (j + 1), OWNED) | within(64 + SLOT * j, OWNED)
            parts.append((mask, lrl(wide[j, wide_at], SLOT * (j + 1) - 32 * p)))
        for j in range(3):
            spot = SLOT * j + OWNED
            both = jnp.where(lane < 64, narrow_in[0, j, narrow_at], narrow_in[1, j, narrow_at])
            mask = within(spot, GHOSTS) | within(64 + spot, GHOSTS)
            parts.append((mask, lrl(both, spot - SLOT * p - 8 * i)))
        return overlay(parts)

    def unpack_early():
        for a, p in tiles():
            value = unpack(P_SIZE + a, PAIRS + a // 2, a % 2, p)
            put(page_rea, a, p, value - shift)
        for f in range(4):
            page_small[f] = unpack(2 * P_SIZE, 2 * PAIRS, 0, f)

    def unpack_late():
        for a, p in tiles():
            put(page_a, a, p, unpack(a, a // 2, a % 2, p))

    def page_level(level):
        given, out = (page_a, page_b) if level % 2 else (page_b, page_a)
        get = functools.partial(tile, given)
        fields = [page_small[f] for f in range(4)]
        fw, fe = xfaces(get)
        if level == 1:
            cw, ce = far_in[0], far_in[1]
            skip = 128 - OWNED
            east = jnp.where(lane < 64, lrl(cw, 3 * SLOT), lrl(cw, 6 * SLOT - skip))
            west = jnp.where(lane < 64, lrl(ce, SLOT), lrl(ce, 4 * SLOT - skip))
            last = within(2 * SLOT + OWNED, SLOT) | within(6 * SLOT, SLOT)
            first = within(OWNED, SLOT) | within(4 * SLOT, SLOT)
        sides = {}
        for p in range(PAIRS):
            e, w = lrl(srl(fw[p], 3), -SLOT), lrl(srl(fe[p], 5), SLOT)
            if level == 1:
                e = jnp.where(last, srl(east, 3 - p), e)
                w = jnp.where(first, srl(west, -p), w)
            nb_e = jnp.where(xpos == 3, e, srl(fw[p], 7))
            nb_w = jnp.where(xpos == 0, w, srl(fe[p], 1))
            sides[0, p] = fw[p] - fields[1] * nb_w
            sides[P_SIZE - 1, p] = fe[p] - fields[2] * nb_e
        own, across = yfaces(get)

        def emit(a, p, value):
            put(out, a, p, value)
            south = lrl(value, -2 * SLOT)
            north = lrl(value, 128 - OWNED - 5 * SLOT)
            patch[level - 1, a * PAIRS + p] = jnp.where(lane < 64, south, north)

        apply(get, functools.partial(tile, page_rea), fields, sides, own, across, emit)

    edge = (lane < VECS) | (lane >= 128 - VECS)

    def patched(level, a, p, v):
        if level == 0:
            return v
        return jnp.where(edge, patch[level - 1, a * PAIRS + p], v)

    started = []

    loads[0].wait()
    get = functools.partial(tile, ini)
    faces = xfaces(get)
    copies = send_halo(0, faces, lambda: pl.semaphore_wait(barrier, n - 1))
    started += copies
    given = yfaces(get)
    send_yfaces(given[1])
    loads[1].wait()
    loads[2].wait()
    operate(get, faces, given, lambda a, p, v: put(bas.at[0], a, p, tile(src, a, p) - v))
    pack_field(rea, P_SIZE, PAIRS)
    pack_small()
    for copy in strip_copies(False):
        copy.start()

    late = gy == ny - 1
    for level in range(ITERS):
        now = bas.at[level]
        get = functools.partial(tile, now)
        fw, fe = xfaces(get)
        first, last = take_halo(level, copies, 1.0 if level == 0 else -1.0)
        fw = [fw[p] + glow[0] * first[p] + glow[P_SIZE - 1] * last[p] for p in range(PAIRS)]
        fe = [fe[p] + gupp[0] * first[p] + gupp[P_SIZE - 1] * last[p] for p in range(PAIRS)]
        copies = send_halo(level + 1, (fw, fe))
        started += copies
        for p in range(PAIRS):
            put(now, 0, p, get(0, p) + first[p])
            put(now, P_SIZE - 1, p, get(P_SIZE - 1, p) + last[p])
        operate(get, (fw, fe), None, functools.partial(put, bas.at[level + 1]))
        if level == 0:
            pl.when(jnp.logical_not(late))(finish_first)
        if level == 1:
            pl.when(late)(finish_first)
            accs = [None] * 3
            for a, p in tiles():
                u, v = tile(bas.at[0], a, p), tile(bas.at[1], a, p)
                new = [u * u, u * v, v * v]
                accs = new if accs[0] is None else [s + t for s, t in zip(accs, new)]
            start_reduce(0, pack_sums(accs, 0))
        if level == 2:
            for copy in strip_copies(False):
                copy.wait_recv()
            unpack_early()
        if level == 3:
            for copy in strip_copies(True):
                copy.wait_recv()
            unpack_late()
            for k in (1, 2, 3):
                page_level(k)
        if level == 4:
            for k in (4, 5):
                page_level(k)

    sums = end_reduce(0)
    size = jnp.maximum(sums(0), 1e-30)
    mean = sums(1) / size
    spread = jnp.sqrt(jnp.maximum(sums(2) / size - mean * mean, 0.0)) + 0.1
    inv = 1.0 / spread
    ratio = mean * inv
    theta = shift + mean
    powers = [None, inv]
    for k in range(2, VECS):
        powers.append(powers[k - 1] * inv)

    pairs = [(i, j) for j in range(ITERS) for i in range(j + 1)]
    accs, tail = None, None
    for a, p in tiles():
        lev = []
        for k in range(VECS):
            v = patched(k, a, p, tile(bas.at[k], a, p))
            lev.append(v if k == 0 else v * powers[k])
        vecs = [lev[0]]
        for k in range(1, VECS):
            lev = [lev[i + 1] - ratio * lev[i] for i in range(len(lev) - 1)]
            vecs.append(lev[0])
        for k in range(1, VECS):
            put(bas.at[k], a, p, vecs[k])
        put(bas.at[0], a, p, vecs[0])
        new = [vecs[i] * vecs[j] for i, j in pairs]
        accs = new if accs is None else [s + t for s, t in zip(accs, new)]
        if 0 < a < P_SIZE - 1:
            new = [v * vecs[ITERS] for v in vecs]
            tail = new if tail is None else [s + t for s, t in zip(tail, new)]
    packed = pack_sums(accs[:8], 0) + pack_sums(accs[8:], 8)

    first, last = take_halo(ITERS, copies, -1.0)
    for a, extra in ((0, first), (P_SIZE - 1, last)):
        for p in range(PAIRS):
            v = tile(bas.at[ITERS], a, p) + jnp.where(edge, 0.0, extra[p] * powers[ITERS])
            put(bas.at[ITERS], a, p, v)
            vecs = [tile(bas.at[k], a, p) for k in range(ITERS)] + [v]
            tail = [s + u * v for s, u in zip(tail, vecs)]
    start_reduce(1, packed + pack_sums(tail, 16))
    sums = end_reduce(1)

    gram = {}
    for k, (i, j) in enumerate(pairs):
        gram[i, j] = sums(k) * (1.0 / total)
    for i in range(VECS):
        gram[i, ITERS] = sums(16 + i) * (1.0 / total)

    def times_gram(u, rows):
        return [
            dot((gram[min(i, r), max(i, r)], u[i]) for i in range(len(u))) for r in range(rows)
        ]

    hess = jnp.zeros((8, 128), jnp.float32)
    combos = [[1.0 / jnp.sqrt(gram[0, 0] + FLOOR)]]
    for j in range(ITERS):
        c = combos[j]
        u = [theta * c[0]]
        for i in range(1, j + 1):
            u.append(spread * c[i - 1] + theta * c[i])
        u.append(spread * c[j])
        g = times_gram(u, j + 1)
        rest = list(u)
        for i in range(j + 1):
            h = dot(zip(combos[i], g))
            hess = jnp.where((sub == i) & (lane == j), h, hess)
            for k in range(i + 1):
                rest[k] = rest[k] - h * combos[i][k]
        square = dot(zip(rest, times_gram(rest, j + 2)))
        beta = jnp.sqrt(jnp.maximum(square, 0.0) + FLOOR)
        hess = jnp.where((sub == j + 1) & (lane == j), beta, hess)
        post = 1.0 / beta
        combos.append([r * post for r in rest])

    for a, p in tiles():
        vecs = [tile(bas.at[k], a, p) for k in range(VECS)]
        for j in reversed(range(VECS)):
            put(bas.at[j], a, p, dot(zip(combos[j], vecs)))
    hess_out[...] = hess[0:VECS, 0:ITERS]

    for copy in started + y_copies() + strip_copies(False) + strip_copies(True):
        copy.wait_send()
    for slot in range(2):
        block = rrecv.at[slot, pl.ds(0, n - 1)]
        pltpu.make_async_copy(block, block, rs_sem.at[slot]).wait()


def store(hess, basis, hess_out, basis_out, sem):
    copies = [
        pltpu.make_async_copy(basis, basis_out, sem.at[0]),
        pltpu.make_async_copy(hess, hess_out, sem.at[1]),
    ]
    for copy in copies:
        copy.start()
    for copy in copies:
        copy.wait()


def body(nx, ny, source, initial, reaction, stiffness, line_op, face_deriv, wall_flags):
    nodes, ex, ey = source.shape
    n = nx * ny
    rows = nodes * ex
    flat = (rows, ey)
    total = float(nodes * ex * nx * ey * ny)
    vmem = pl.BlockSpec(memory_space=pltpu.VMEM)
    hbm = pl.BlockSpec(memory_space=pl.ANY)
    smem = pl.BlockSpec(memory_space=pltpu.SMEM)

    def array(*lead):
        return pltpu.VMEM(lead + (8, 128), jnp.float32)

    dma = pltpu.SemaphoreType.DMA
    hess, basis = pl.pallas_call(
        functools.partial(kernel, nx, ny, total),
        out_shape=(
            pltpu.VMEM((VECS, ITERS), jnp.float32),
            pltpu.VMEM((VECS,) + flat, jnp.float32),
        ),
        in_specs=[smem, smem, hbm, hbm, hbm, vmem, vmem],
        out_specs=(vmem, vmem),
        scratch_shapes=[
            array(2 * PAIRS * PAIRS),
            array(2 * PAIRS),
            array(4),
            pltpu.VMEM(flat, jnp.float32),
            pltpu.VMEM(flat, jnp.float32),
            pltpu.VMEM(flat, jnp.float32),
            array(3, WIDE),
            array(NARROW),
            array(2, 3, NARROW),
            array(2),
            array(2),
            pltpu.VMEM(flat, jnp.float32),
            array(4),
            pltpu.VMEM(flat, jnp.float32),
            pltpu.VMEM(flat, jnp.float32),
            array(ITERS, P_SIZE * PAIRS),
            dma((3,)),
            array(VECS, 2),
            array(VECS, 2),
            array(),
            array(2),
            pltpu.VMEM((2, 1, 128), jnp.float32),
            pltpu.VMEM((2, n, 128), jnp.float32),
            dma((VECS, 2)),
            dma((VECS, 2)),
            dma((2,)),
            dma((2,)),
            dma((2, 3)),
            dma((2, 3)),
            dma((2, 2, 3)),
            dma((2, 2, 3)),
            dma((2,)),
            dma((2,)),
            dma((2,)),
            dma((2,)),
        ],
        compiler_params=pltpu.CompilerParams(collective_id=0, has_side_effects=True),
    )(
        line_op, face_deriv, source.reshape(flat), initial.reshape(flat), reaction.reshape(flat),
        stiffness, wall_flags,
    )
    hess = pltpu.with_memory_space_constraint(hess, pltpu.VMEM)
    basis = pltpu.with_memory_space_constraint(basis, pltpu.VMEM)
    hess, basis = pl.pallas_call(
        store,
        out_shape=(
            jax.ShapeDtypeStruct(hess.shape, jnp.float32),
            jax.ShapeDtypeStruct(basis.shape, jnp.float32),
        ),
        in_specs=[hbm, hbm],
        out_specs=(hbm, hbm),
        scratch_shapes=[pltpu.SemaphoreType.DMA((2,))],
    )(hess, basis)
    return hess, basis.reshape((VECS, nodes, ex, ey))


def solution(mesh):
    return jax.shard_map(
        functools.partial(body, mesh.shape["gx"], mesh.shape["gy"]),
        mesh=mesh,
        in_specs=(
            P(None, "gx", "gy"),
            P(None, "gx", "gy"),
            P(None, "gx", "gy"),
            P("gx", "gy"),
            P(),
            P(),
            P(None, "gx", "gy"),
        ),
        out_specs=(P(), P(None, None, "gx", "gy")),
        check_vma=False,
    )
```

```python
import functools

import jax
import jax.numpy as jnp
from jax import lax
from jax.experimental import pallas as pl
from jax.experimental.pallas import tpu as pltpu
from jax.sharding import PartitionSpec as P

P_SIZE = 8
ITERS = 5
VECS = ITERS + 1
TAU = 2.0
FLOOR = 0.1
PAIRS = P_SIZE // 2
SLOT = 16
GHOSTS = ITERS
OWNED = SLOT - GHOSTS
WIDE = 2 * P_SIZE + 1
NARROW = P_SIZE + 1
MESH = pl.DeviceIdType.MESH


def kernel(
    nx, ny, total,
    line_any, deriv_any, src_any, ini_any, rea_any, stf_any, wal_any,
    hess_out, bas,
    line, deriv, stf, wal, coef, gcoef, small, src, ini, rea,
    wide, narrow, narrow_in, far_send, far_in,
    page_rea, page_small, page_a, page_b, patch,
    in_sem, hsend, hrecv, ysend, yrecv, rsend, rrecv,
    hs_sem, hr_sem, ys_sem, yr_sem, ws_sem, wr_sem, ns_sem, nr_sem,
    fs_sem, fr_sem, rs_sem, rr_sem,
):
    n = nx * ny
    gx, gy = lax.axis_index("gx"), lax.axis_index("gy")
    me = gx * ny + gy

    side = gy // (ny // 2)
    offsets = sorted(range(1, nx), key=lambda d: abs(2 * d - nx))

    def for_peers(act):
        def column(k, own_column):
            across = side * k + (1 - side) * (ny - 1 - k)
            for d in offsets:
                act((lax.rem(gx + d, nx), across))
            if own_column:
                skip = jnp.where(k >= (side * gy + (1 - side) * (ny - 1 - gy)), 1, 0)
                act((gx, across + (2 * side - 1) * skip))

        if n <= 64:
            for k in range(ny - 1):
                column(k, True)
        else:
            lax.fori_loop(0, ny - 1, lambda k, c: (column(k, True), c)[1], 0)
        column(ny - 1, False)

    def at(dx, dy):
        return (lax.rem(gx + dx + nx, nx), lax.rem(gy + dy + ny, ny))

    barrier = pltpu.get_barrier_semaphore()

    def greet(device):
        pl.semaphore_signal(barrier, inc=1, device_id=device, device_id_type=MESH)

    loads = [
        pltpu.make_async_copy(given, held, in_sem.at[k])
        for k, (given, held) in enumerate((
            (ini_any, ini), (line_any, line), (deriv_any, deriv), (stf_any, stf),
            (wal_any, wal), (src_any, src), (rea_any, rea),
        ))
    ]
    for load in loads:
        load.start()
    for_peers(greet)
    for load in loads[1:5]:
        load.wait()

    sub = lax.broadcasted_iota(jnp.int32, (8, 128), 0)
    lane = lax.broadcasted_iota(jnp.int32, (8, 128), 1)
    low = sub < 4
    xpos = sub % 4
    def srl(v, s):
        s = s % 8
        return v if s == 0 else pltpu.roll(v, s, 0)

    def lrl(v, s):
        s = s % 128
        return v if s == 0 else pltpu.roll(v, s, 1)

    def halves(a, b):
        return jnp.where(low, a, b)

    def within(start, count):
        return (lane >= start) & (lane < start + count)

    def overlay(parts):
        out = None
        for mask, v in parts:
            out = v if out is None else jnp.where(mask, v, out)
        return out

    def dot(pairs):
        out = None
        for c, v in pairs:
            out = c * v if out is None else out + c * v
        return out

    for p in range(PAIRS):
        for r in range(PAIRS):
            k = (p * PAIRS + r) * 2
            coef[k] = halves(line[2 * p, 2 * r], line[2 * p + 1, 2 * r + 1])
            coef[k + 1] = halves(line[2 * p, 2 * r + 1], line[2 * p + 1, 2 * r])
    glow = [0.5 * deriv[c] + (TAU if c == 0 else 0.0) for c in range(P_SIZE)]
    gupp = [
        0.5 * deriv[P_SIZE - 1 - c] + (TAU if c == P_SIZE - 1 else 0.0) for c in range(P_SIZE)
    ]
    for p in range(PAIRS):
        gcoef[p] = halves(glow[2 * p], glow[2 * p + 1])
        gcoef[PAIRS + p] = halves(gupp[2 * p], gupp[2 * p + 1])
    small[0, 0:4] = stf[...]
    small[0, 4:8] = stf[...]
    opened = [1.0 - wal[f].astype(jnp.float32) for f in range(4)]
    for slot, (first, second) in enumerate(((0, 0), (1, 1), (2, 3))):
        small[slot + 1, 0:4] = opened[first]
        small[slot + 1, 4:8] = opened[second]
    trace = line[0, 0]
    for c in range(1, P_SIZE):
        trace = trace + line[c, c]
    shift = 3.0 + 0.25 * trace

    def tile(ref, a, p):
        return ref[pl.ds((a * PAIRS + p) * 8, 8), :]

    def put(ref, a, p, value):
        ref[pl.ds((a * PAIRS + p) * 8, 8), :] = value

    def tiles():
        return [(a, p) for a in range(P_SIZE) for p in range(PAIRS)]

    def xfaces(get):
        fw, fe = [], []
        for p in range(PAIRS):
            vs = [get(c, p) for c in range(P_SIZE)]
            fw.append(dot(zip(glow, vs)))
            fe.append(dot(zip(gupp, vs)))
        return fw, fe

    def halo_copy(slot, way, device):
        rows = pl.ds(0, 3 if slot == 0 else 2)
        return pltpu.make_async_remote_copy(
            src_ref=hsend.at[slot, way, rows],
            dst_ref=hrecv.at[slot, way, rows],
            send_sem=hs_sem.at[slot, way],
            recv_sem=hr_sem.at[slot, way],
            device_id=device,
            device_id_type=MESH,
        )

    def pack_faces(faces):
        fw, fe = faces
        cw, ce = fw[0], srl(fe[0], -3)
        for p in range(1, PAIRS):
            cw = jnp.where(xpos == p, srl(fw[p], p), cw)
            ce = jnp.where(xpos == p, srl(fe[p], p - 3), ce)
        return cw, ce

    def halo_copies(slot):
        return [halo_copy(slot, 0, at(-1, 0)), halo_copy(slot, 1, at(1, 0))]

    def send_halo(slot, faces, ahead, ready=lambda: None):
        for k, pair in enumerate((pack_faces(faces), pack_faces(ahead))):
            for way in range(2):
                hsend[slot, way, k] = pair[way]
        if slot == 0:
            hsend[0, 0, 2] = jnp.broadcast_to(small[1, 0:1], (8, 128))
            hsend[0, 1, 2] = jnp.broadcast_to(small[2, 3:4], (8, 128))
        ready()
        for copy in halo_copies(slot):
            copy.start()

    def inject(cw, ce, sign):
        open_w, open_e = small[1] * sign, small[2] * sign
        first = [open_w * jnp.where(xpos == 0, srl(ce, -p), 0.0) for p in range(PAIRS)]
        last = [open_e * jnp.where(xpos == 3, srl(cw, 3 - p), 0.0) for p in range(PAIRS)]
        return first, last

    def take_halo(slot, sign):
        for copy in halo_copies(slot):
            copy.wait_recv()
        cw, ce = hrecv[slot, 0, 0], hrecv[slot, 1, 0]
        own_w, own_e = hsend[slot, 0, 0], hsend[slot, 1, 0]
        ahead_w = hrecv[slot, 0, 1] + (glow[0] * sign) * (hrecv[0, 0, 2] * own_e)
        ahead_e = hrecv[slot, 1, 1] + (gupp[P_SIZE - 1] * sign) * (hrecv[0, 1, 2] * own_w)
        return inject(cw, ce, sign), inject(ahead_w, ahead_e, -1.0)

    edge_lane = lane == jnp.where(low, 0, 127)

    def yfaces(get):
        own, across = [], []
        for a in range(P_SIZE):
            vs = [get(a, p) for p in range(PAIRS)]
            s = dot((gcoef[p], vs[p]) for p in range(PAIRS))
            t = dot((gcoef[PAIRS + p], vs[p]) for p in range(PAIRS))
            u = halves(s, t) + srl(halves(t, s), 4)
            q = srl(u, 4)
            own.append(u)
            across.append(halves(lrl(q, 1), lrl(q, 127)))
        return own, across

    def y_copy(target, device):
        return pltpu.make_async_remote_copy(
            src_ref=ysend,
            dst_ref=yrecv.at[target],
            send_sem=ys_sem.at[target],
            recv_sem=yr_sem.at[target],
            device_id=device,
            device_id_type=MESH,
        )

    def y_copies():
        return [y_copy(0, at(0, 1)), y_copy(1, at(0, -1))]

    def send_yfaces(across):
        packed = across[0]
        for a in range(1, P_SIZE):
            mask = lane == jnp.where(low, a, a - 1)
            packed = jnp.where(mask, lrl(across[a], a), packed)
        ysend[...] = packed
        for copy in y_copies():
            copy.start()

    def apply(get, react, fields, sides, own, across, emit):
        stiff, open_w, open_e, open_y = fields
        for a in range(P_SIZE):
            vs = [get(a, p) for p in range(PAIRS)]
            ss = [srl(v, 4) for v in vs]
            term = own[a] - open_y * across[a]
            for p in range(PAIRS):
                acc = None
                for r in range(PAIRS):
                    k = (p * PAIRS + r) * 2
                    part = coef[k] * vs[r] + coef[k + 1] * ss[r]
                    acc = part if acc is None else acc + part
                other = dot((line[a, c], get(c, p)) for c in range(P_SIZE))
                value = react(a, p) * vs[p] + stiff * (acc + other)
                if p == 0:
                    value = value + jnp.where(low, term, 0.0)
                if p == PAIRS - 1:
                    value = value + jnp.where(low, 0.0, term)
                if (a, p) in sides:
                    value = value + sides[a, p]
                emit(a, p, value)

    def operate(get, faces, given, emit):
        fw, fe = faces
        fields = [small[f] for f in range(4)]
        sides = {}
        for p in range(PAIRS):
            nb_e = jnp.where(xpos == 3, 0.0, srl(fw[p], 7))
            nb_w = jnp.where(xpos == 0, 0.0, srl(fe[p], 1))
            sides[0, p] = fw[p] - fields[1] * nb_w
            sides[P_SIZE - 1, p] = fe[p] - fields[2] * nb_e
        own, across = given or yfaces(get)
        if given:
            across = [jnp.where(edge_lane, 0.0, v) for v in across]
            react = functools.partial(tile, rea)
        else:
            react = lambda a, p: tile(rea, a, p) - shift
        apply(get, react, fields, sides, own, across, emit)

    def gather_rows(accs):
        zero = jnp.zeros((8, 128), jnp.float32)
        level = list(accs) + [zero] * (8 - len(accs))
        for step in (1, 2, 4):
            keep = (sub // step) % 2 == 0
            level = [
                jnp.where(keep, level[i], level[i + 1])
                + srl(jnp.where(keep, level[i + 1], level[i]), step)
                for i in range(0, len(level), 2)
            ]
        return level[0]

    def fold(v):
        for step in (4, 2, 1):
            v = v + srl(v, step)
        return v

    def row_copy(slot, device):
        return pltpu.make_async_remote_copy(
            src_ref=rsend.at[slot],
            dst_ref=rrecv.at[slot, pl.ds(me, 1)],
            send_sem=rs_sem.at[slot],
            recv_sem=rr_sem.at[slot],
            device_id=device,
            device_id_type=MESH,
        )

    def pack_sums(accs, start):
        sums = jnp.sum(gather_rows(accs), axis=1, keepdims=True)
        return jnp.where(lane == sub + start, sums, 0.0)

    def start_reduce(slot, packed):
        row = fold(packed)[0:1]
        rsend[slot] = row
        rrecv[slot, pl.ds(me, 1)] = row
        for_peers(lambda device: row_copy(slot, device).start())

    def end_reduce(slot):
        block = rrecv.at[slot, pl.ds(0, n - 1)]
        pltpu.make_async_copy(block, block, rr_sem.at[slot]).wait()
        value = rrecv[slot, 0:8]
        for g in range(1, n // 8):
            value = value + rrecv[slot, 8 * g:8 * g + 8]
        value = fold(value)
        return lambda k: jnp.broadcast_to(value[:, k:k + 1], (8, 128))

    near = (-1, 0, 1)

    def narrow_copy(late, o, dy):
        rows = pl.ds(0, PAIRS) if late else pl.ds(PAIRS, PAIRS + 1)
        side, j = (0 if dy > 0 else 1), near.index(-o)
        sems = (1 if late else 0, side, j)
        return pltpu.make_async_remote_copy(
            src_ref=narrow.at[rows],
            dst_ref=narrow_in.at[side, j, rows],
            send_sem=ns_sem.at[sems],
            recv_sem=nr_sem.at[sems],
            device_id=at(o, dy),
            device_id_type=MESH,
        )

    def wide_copy(late, o):
        rows = pl.ds(0, P_SIZE) if late else pl.ds(P_SIZE, P_SIZE + 1)
        j = near.index(-o)
        sems = (1 if late else 0, j)
        return pltpu.make_async_remote_copy(
            src_ref=wide.at[1, rows],
            dst_ref=wide.at[j, rows],
            send_sem=ws_sem.at[sems],
            recv_sem=wr_sem.at[sems],
            device_id=at(o, 0),
            device_id_type=MESH,
        )

    def far_copy(way, o):
        return pltpu.make_async_remote_copy(
            src_ref=far_send.at[way],
            dst_ref=far_in.at[way],
            send_sem=fs_sem.at[way],
            recv_sem=fr_sem.at[way],
            device_id=at(o, 0),
            device_id_type=MESH,
        )

    def strip_copies(late):
        copies = [narrow_copy(late, o, dy) for dy in (-1, 1) for o in near]
        copies += [wide_copy(late, o) for o in (-1, 1)]
        if late:
            copies += [far_copy(0, -2), far_copy(1, 2)]
        return copies

    def pack_wide(items, index):
        parts = []
        for p, v in enumerate(items):
            parts.append((within(32 * p, SLOT), lrl(v, 32 * p)))
            spot = (32 * p + 48) % 128
            parts.append((within(spot, SLOT), lrl(v, spot - (128 - OWNED))))
        wide[1, index] = overlay(parts)

    def pack_narrow(pairs, index):
        parts = []
        for i, items in enumerate(pairs):
            for p, v in enumerate(items):
                spot = SLOT * p + 8 * i
                parts.append((within(spot, 8), lrl(v, spot - (128 - GHOSTS))))
                parts.append((within(64 + spot, 8), lrl(v, 64 + spot)))
        narrow[index] = overlay(parts)

    def pack_field(ref, wide_at, narrow_at):
        rows = [[tile(ref, a, p) for p in range(PAIRS)] for a in range(P_SIZE)]
        for a in range(P_SIZE):
            pack_wide(rows[a], wide_at + a)
        for q in range(PAIRS):
            pack_narrow(rows[2 * q:2 * q + 2], narrow_at + q)

    def pack_small():
        items = [small[f] for f in range(4)]
        pack_wide(items, 2 * P_SIZE)
        pack_narrow([items], 2 * PAIRS)

    def finish_first():
        for copy in y_copies():
            copy.wait_recv()
        cy = halves(yrecv[0], yrecv[1])
        first = bas.at[0]
        for a in range(P_SIZE):
            term = small[3] * jnp.where(edge_lane, lrl(cy, -a), 0.0)
            put(first, a, 0, tile(first, a, 0) + jnp.where(low, term, 0.0))
            last = PAIRS - 1
            put(first, a, last, tile(first, a, last) + jnp.where(low, 0.0, term))
        cw, ce = pack_faces(xfaces(functools.partial(tile, first)))
        far_send[0] = cw
        far_send[1] = ce
        pack_field(first, 0, 0)
        for copy in strip_copies(True):
            copy.start()

    def unpack(wide_at, narrow_at, i, p):
        parts = []
        for j in range(3):
            mask = within(SLOT * (j + 1), OWNED) | within(64 + SLOT * j, OWNED)
            parts.append((mask, lrl(wide[j, wide_at], SLOT * (j + 1) - 32 * p)))
        for j in range(3):
            spot = SLOT * j + OWNED
            both = jnp.where(lane < 64, narrow_in[0, j, narrow_at], narrow_in[1, j, narrow_at])
            mask = within(spot, GHOSTS) | within(64 + spot, GHOSTS)
            parts.append((mask, lrl(both, spot - SLOT * p - 8 * i)))
        return overlay(parts)

    def unpack_early():
        for a, p in tiles():
            value = unpack(P_SIZE + a, PAIRS + a // 2, a % 2, p)
            put(page_rea, a, p, value - shift)
        for f in range(4):
            page_small[f] = unpack(2 * P_SIZE, 2 * PAIRS, 0, f)

    def unpack_late():
        for a, p in tiles():
            put(page_a, a, p, unpack(a, a // 2, a % 2, p))

    def page_level(level):
        given, out = (page_a, page_b) if level % 2 else (page_b, page_a)
        get = functools.partial(tile, given)
        fields = [page_small[f] for f in range(4)]
        fw, fe = xfaces(get)
        if level == 1:
            cw, ce = far_in[0], far_in[1]
            skip = 128 - OWNED
            east = jnp.where(lane < 64, lrl(cw, 3 * SLOT), lrl(cw, 6 * SLOT - skip))
            west = jnp.where(lane < 64, lrl(ce, SLOT), lrl(ce, 4 * SLOT - skip))
            last = within(2 * SLOT + OWNED, SLOT) | within(6 * SLOT, SLOT)
            first = within(OWNED, SLOT) | within(4 * SLOT, SLOT)
        sides = {}
        for p in range(PAIRS):
            e, w = lrl(srl(fw[p], 3), -SLOT), lrl(srl(fe[p], 5), SLOT)
            if level == 1:
                e = jnp.where(last, srl(east, 3 - p), e)
                w = jnp.where(first, srl(west, -p), w)
            nb_e = jnp.where(xpos == 3, e, srl(fw[p], 7))
            nb_w = jnp.where(xpos == 0, w, srl(fe[p], 1))
            sides[0, p] = fw[p] - fields[1] * nb_w
            sides[P_SIZE - 1, p] = fe[p] - fields[2] * nb_e
        own, across = yfaces(get)

        def emit(a, p, value):
            put(out, a, p, value)
            south = lrl(value, -2 * SLOT)
            north = lrl(value, 128 - OWNED - 5 * SLOT)
            patch[level - 1, a * PAIRS + p] = jnp.where(lane < 64, south, north)

        apply(get, functools.partial(tile, page_rea), fields, sides, own, across, emit)

    edge = (lane < VECS) | (lane >= 128 - VECS)

    def patched(level, a, p, v):
        if level == 0:
            return v
        return jnp.where(edge, patch[level - 1, a * PAIRS + p], v)

    def finish_rows(ref, first, last):
        for p in range(PAIRS):
            put(ref, 0, p, tile(ref, 0, p) + first[p])
            put(ref, P_SIZE - 1, p, tile(ref, P_SIZE - 1, p) + last[p])

    loads[0].wait()
    get = functools.partial(tile, ini)
    faces = xfaces(get)
    given = yfaces(get)
    loads[5].wait()
    loads[6].wait()
    operate(get, faces, given, lambda a, p, v: put(bas.at[0], a, p, tile(src, a, p) - v))

    late = gy == ny - 1
    for step in range(VECS // 2):
        now, after = bas.at[2 * step], bas.at[2 * step + 1]
        fw, fe = xfaces(functools.partial(tile, now))
        if step == 0:
            send_halo(0, faces, (fw, fe), lambda: pl.semaphore_wait(barrier, n - 1))
            send_yfaces(given[1])
            pack_field(rea, P_SIZE, PAIRS)
            pack_small()
            for copy in strip_copies(False):
                copy.start()
        else:
            send_halo(step, faces, (fw, fe))
        if step == 1:
            pl.when(jnp.logical_not(late))(finish_first)
            accs = [None] * 3
            for a, p in tiles():
                u, v = tile(bas.at[0], a, p), tile(bas.at[1], a, p)
                new = [u * u, u * v, v * v]
                accs = new if accs[0] is None else [s + t for s, t in zip(accs, new)]
            start_reduce(0, pack_sums(accs, 0))
        if step == 2:
            pl.when(late)(finish_first)
            for copy in strip_copies(False):
                copy.wait_recv()
            unpack_early()
        (first, last), extra = take_halo(step, 1.0 if step == 0 else -1.0)
        fw = [fw[p] + glow[0] * first[p] + glow[P_SIZE - 1] * last[p] for p in range(PAIRS)]
        fe = [fe[p] + gupp[0] * first[p] + gupp[P_SIZE - 1] * last[p] for p in range(PAIRS)]
        finish_rows(now, first, last)
        operate(functools.partial(tile, now), (fw, fe), None, functools.partial(put, after))
        finish_rows(after, *extra)
        if step < VECS // 2 - 1:
            get = functools.partial(tile, after)
            faces = xfaces(get)
            operate(get, faces, None, functools.partial(put, bas.at[2 * step + 2]))

    for copy in strip_copies(True):
        copy.wait_recv()
    unpack_late()
    for k in range(1, VECS):
        page_level(k)

    sums = end_reduce(0)
    size = jnp.maximum(sums(0), 1e-30)
    mean = sums(1) / size
    spread = jnp.sqrt(jnp.maximum(sums(2) / size - mean * mean, 0.0)) + 0.1
    inv = 1.0 / spread
    ratio = mean * inv
    theta = shift + mean
    powers = [None, inv]
    for k in range(2, VECS):
        powers.append(powers[k - 1] * inv)

    pairs = [(i, j) for j in range(VECS) for i in range(j + 1)]
    accs = None
    for a, p in tiles():
        lev = []
        for k in range(VECS):
            v = patched(k, a, p, tile(bas.at[k], a, p))
            lev.append(v if k == 0 else v * powers[k])
        vecs = [lev[0]]
        for k in range(1, VECS):
            lev = [lev[i + 1] - ratio * lev[i] for i in range(len(lev) - 1)]
            vecs.append(lev[0])
        for k in range(1, VECS):
            put(bas.at[k], a, p, vecs[k])
        new = [vecs[i] * vecs[j] for i, j in pairs]
        accs = new if accs is None else [s + t for s, t in zip(accs, new)]
    packed = pack_sums(accs[:8], 0) + pack_sums(accs[8:16], 8) + pack_sums(accs[16:], 16)
    start_reduce(1, packed)
    sums = end_reduce(1)

    gram = {}
    for k, (i, j) in enumerate(pairs):
        gram[i, j] = sums(k) * (1.0 / total)
    def times_gram(u, rows):
        return [
            dot((gram[min(i, r), max(i, r)], u[i]) for i in range(len(u))) for r in range(rows)
        ]

    hess = jnp.zeros((8, 128), jnp.float32)
    combos = [[1.0 / jnp.sqrt(gram[0, 0] + FLOOR)]]
    for j in range(ITERS):
        c = combos[j]
        u = [theta * c[0]]
        for i in range(1, j + 1):
            u.append(spread * c[i - 1] + theta * c[i])
        u.append(spread * c[j])
        g = times_gram(u, j + 1)
        rest = list(u)
        for i in range(j + 1):
            h = dot(zip(combos[i], g))
            hess = jnp.where((sub == i) & (lane == j), h, hess)
            for k in range(i + 1):
                rest[k] = rest[k] - h * combos[i][k]
        square = dot(zip(rest, times_gram(rest, j + 2)))
        beta = jnp.sqrt(jnp.maximum(square, 0.0) + FLOOR)
        hess = jnp.where((sub == j + 1) & (lane == j), beta, hess)
        post = 1.0 / beta
        combos.append([r * post for r in rest])

    for a, p in tiles():
        vecs = [tile(bas.at[k], a, p) for k in range(VECS)]
        for j in reversed(range(VECS)):
            put(bas.at[j], a, p, dot(zip(combos[j], vecs)))
    hess_out[...] = hess[0:VECS, 0:ITERS]

    halos = [copy for slot in range(VECS // 2) for copy in halo_copies(slot)]
    for copy in halos + y_copies() + strip_copies(False) + strip_copies(True):
        copy.wait_send()
    for slot in range(2):
        block = rrecv.at[slot, pl.ds(0, n - 1)]
        pltpu.make_async_copy(block, block, rs_sem.at[slot]).wait()


def store(hess, basis, hess_out, basis_out, sem):
    copies = [
        pltpu.make_async_copy(basis, basis_out, sem.at[0]),
        pltpu.make_async_copy(hess, hess_out, sem.at[1]),
    ]
    for copy in copies:
        copy.start()
    for copy in copies:
        copy.wait()


def body(nx, ny, source, initial, reaction, stiffness, line_op, face_deriv, wall_flags):
    nodes, ex, ey = source.shape
    n = nx * ny
    rows = nodes * ex
    flat = (rows, ey)
    total = float(nodes * ex * nx * ey * ny)
    vmem = pl.BlockSpec(memory_space=pltpu.VMEM)
    hbm = pl.BlockSpec(memory_space=pl.ANY)

    def array(*lead):
        return pltpu.VMEM(lead + (8, 128), jnp.float32)

    dma = pltpu.SemaphoreType.DMA
    hess, basis = pl.pallas_call(
        functools.partial(kernel, nx, ny, total),
        out_shape=(
            pltpu.VMEM((VECS, ITERS), jnp.float32),
            pltpu.VMEM((VECS,) + flat, jnp.float32),
        ),
        in_specs=[hbm] * 7,
        out_specs=(vmem, vmem),
        scratch_shapes=[
            pltpu.SMEM(line_op.shape, jnp.float32),
            pltpu.SMEM(face_deriv.shape, jnp.float32),
            pltpu.VMEM(stiffness.shape, jnp.float32),
            pltpu.VMEM(wall_flags.shape, wall_flags.dtype),
            array(2 * PAIRS * PAIRS),
            array(2 * PAIRS),
            array(4),
            pltpu.VMEM(flat, jnp.float32),
            pltpu.VMEM(flat, jnp.float32),
            pltpu.VMEM(flat, jnp.float32),
            array(3, WIDE),
            array(NARROW),
            array(2, 3, NARROW),
            array(2),
            array(2),
            pltpu.VMEM(flat, jnp.float32),
            array(4),
            pltpu.VMEM(flat, jnp.float32),
            pltpu.VMEM(flat, jnp.float32),
            array(ITERS, P_SIZE * PAIRS),
            dma((7,)),
            array(VECS // 2, 2, 3),
            array(VECS // 2, 2, 3),
            array(),
            array(2),
            pltpu.VMEM((2, 1, 128), jnp.float32),
            pltpu.VMEM((2, n, 128), jnp.float32),
            dma((VECS // 2, 2)),
            dma((VECS // 2, 2)),
            dma((2,)),
            dma((2,)),
            dma((2, 3)),
            dma((2, 3)),
            dma((2, 2, 3)),
            dma((2, 2, 3)),
            dma((2,)),
            dma((2,)),
            dma((2,)),
            dma((2,)),
        ],
        compiler_params=pltpu.CompilerParams(collective_id=0, has_side_effects=True),
    )(
        line_op, face_deriv, source.reshape(flat), initial.reshape(flat), reaction.reshape(flat),
        stiffness, wall_flags,
    )
    hess = pltpu.with_memory_space_constraint(hess, pltpu.VMEM)
    basis = pltpu.with_memory_space_constraint(basis, pltpu.VMEM)
    hess, basis = pl.pallas_call(
        store,
        out_shape=(
            jax.ShapeDtypeStruct(hess.shape, jnp.float32),
            jax.ShapeDtypeStruct(basis.shape, jnp.float32),
        ),
        in_specs=[hbm, hbm],
        out_specs=(hbm, hbm),
        scratch_shapes=[pltpu.SemaphoreType.DMA((2,))],
    )(hess, basis)
    return hess, basis.reshape((VECS, nodes, ex, ey))


def solution(mesh):
    return jax.shard_map(
        functools.partial(body, mesh.shape["gx"], mesh.shape["gy"]),
        mesh=mesh,
        in_specs=(
            P(None, "gx", "gy"),
            P(None, "gx", "gy"),
            P(None, "gx", "gy"),
            P("gx", "gy"),
            P(),
            P(),
            P(None, "gx", "gy"),
        ),
        out_specs=(P(), P(None, None, "gx", "gy")),
        check_vma=False,
    )
```

```python
import functools

import jax
import jax.numpy as jnp
from jax import lax
from jax.experimental import pallas as pl
from jax.experimental.pallas import tpu as pltpu
from jax.sharding import PartitionSpec as P

P_SIZE = 8
ITERS = 5
VECS = ITERS + 1
TAU = 2.0
FLOOR = 0.1
PAIRS = P_SIZE // 2
SLOT = 16
GHOSTS = ITERS
OWNED = SLOT - GHOSTS
WIDE = 2 * P_SIZE + 1
NARROW = P_SIZE + 1
MESH = pl.DeviceIdType.MESH


def kernel(
    nx, ny, total,
    line_any, deriv_any, src_any, ini_any, rea_any, stf_any, wal_any,
    hess_out, bas,
    line, deriv, stf, wal, coef, gcoef, small, src, ini, rea,
    wide, narrow, narrow_in, far_send, far_in,
    page_rea, page_small, page_a, page_b, patch,
    in_sem, hsend, hrecv, ysend, yrecv, rsend, rrecv,
    hs_sem, hr_sem, ys_sem, yr_sem, ws_sem, wr_sem, ns_sem, nr_sem,
    fs_sem, fr_sem, rs_sem, rr_sem,
):
    n = nx * ny
    gx, gy = lax.axis_index("gx"), lax.axis_index("gy")
    me = gx * ny + gy

    side = gy // (ny // 2)
    offsets = sorted(range(1, nx), key=lambda d: abs(2 * d - nx))

    def for_peers(act):
        def column(k, own_column):
            across = side * k + (1 - side) * (ny - 1 - k)
            for d in offsets:
                act((lax.rem(gx + d, nx), across))
            if own_column:
                skip = jnp.where(k >= (side * gy + (1 - side) * (ny - 1 - gy)), 1, 0)
                act((gx, across + (2 * side - 1) * skip))

        if n <= 64:
            for k in range(ny - 1):
                column(k, True)
        else:
            lax.fori_loop(0, ny - 1, lambda k, c: (column(k, True), c)[1], 0)
        column(ny - 1, False)

    def at(dx, dy):
        return (lax.rem(gx + dx + nx, nx), lax.rem(gy + dy + ny, ny))

    barrier = pltpu.get_barrier_semaphore()

    def greet(device):
        pl.semaphore_signal(barrier, inc=1, device_id=device, device_id_type=MESH)

    loads = [
        pltpu.make_async_copy(given, held, in_sem.at[k])
        for k, (given, held) in enumerate((
            (ini_any, ini), (line_any, line), (deriv_any, deriv), (stf_any, stf),
            (wal_any, wal), (src_any, src), (rea_any, rea),
        ))
    ]
    for load in loads:
        load.start()
    for_peers(greet)
    for load in loads[1:5]:
        load.wait()

    sub = lax.broadcasted_iota(jnp.int32, (8, 128), 0)
    lane = lax.broadcasted_iota(jnp.int32, (8, 128), 1)
    low = sub < 4
    xpos = sub % 4
    def srl(v, s):
        s = s % 8
        return v if s == 0 else pltpu.roll(v, s, 0)

    def lrl(v, s):
        s = s % 128
        return v if s == 0 else pltpu.roll(v, s, 1)

    def halves(a, b):
        return jnp.where(low, a, b)

    def within(start, count):
        return (lane >= start) & (lane < start + count)

    def overlay(parts):
        out = None
        for mask, v in parts:
            out = v if out is None else jnp.where(mask, v, out)
        return out

    def dot(pairs):
        out = None
        for c, v in pairs:
            out = c * v if out is None else out + c * v
        return out

    for p in range(PAIRS):
        for r in range(PAIRS):
            k = (p * PAIRS + r) * 2
            coef[k] = halves(line[2 * p, 2 * r], line[2 * p + 1, 2 * r + 1])
            coef[k + 1] = halves(line[2 * p, 2 * r + 1], line[2 * p + 1, 2 * r])
    glow = [0.5 * deriv[c] + (TAU if c == 0 else 0.0) for c in range(P_SIZE)]
    gupp = [
        0.5 * deriv[P_SIZE - 1 - c] + (TAU if c == P_SIZE - 1 else 0.0) for c in range(P_SIZE)
    ]
    for p in range(PAIRS):
        gcoef[p] = halves(glow[2 * p], glow[2 * p + 1])
        gcoef[PAIRS + p] = halves(gupp[2 * p], gupp[2 * p + 1])
    small[0, 0:4] = stf[...]
    small[0, 4:8] = stf[...]
    opened = [1.0 - wal[f].astype(jnp.float32) for f in range(4)]
    for slot, (first, second) in enumerate(((0, 0), (1, 1), (2, 3))):
        small[slot + 1, 0:4] = opened[first]
        small[slot + 1, 4:8] = opened[second]
    trace = line[0, 0]
    for c in range(1, P_SIZE):
        trace = trace + line[c, c]
    shift = 3.0 + 0.25 * trace

    def tile(ref, a, p):
        return ref[pl.ds((a * PAIRS + p) * 8, 8), :]

    def put(ref, a, p, value):
        ref[pl.ds((a * PAIRS + p) * 8, 8), :] = value

    def tiles():
        return [(a, p) for a in range(P_SIZE) for p in range(PAIRS)]

    def xfaces(get):
        fw, fe = [], []
        for p in range(PAIRS):
            vs = [get(c, p) for c in range(P_SIZE)]
            fw.append(dot(zip(glow, vs)))
            fe.append(dot(zip(gupp, vs)))
        return fw, fe

    def halo_copy(slot, way, device):
        rows = pl.ds(0, 3 if slot == 0 else 2)
        return pltpu.make_async_remote_copy(
            src_ref=hsend.at[slot, way, rows],
            dst_ref=hrecv.at[slot, way, rows],
            send_sem=hs_sem.at[slot, way],
            recv_sem=hr_sem.at[slot, way],
            device_id=device,
            device_id_type=MESH,
        )

    def pack_faces(faces):
        fw, fe = faces
        cw, ce = fw[0], srl(fe[0], -3)
        for p in range(1, PAIRS):
            cw = jnp.where(xpos == p, srl(fw[p], p), cw)
            ce = jnp.where(xpos == p, srl(fe[p], p - 3), ce)
        return cw, ce

    def halo_copies(slot):
        return [halo_copy(slot, 0, at(-1, 0)), halo_copy(slot, 1, at(1, 0))]

    def send_halo(slot, faces, ahead, ready=lambda: None):
        for k, pair in enumerate((pack_faces(faces), pack_faces(ahead))):
            for way in range(2):
                hsend[slot, way, k] = pair[way]
        if slot == 0:
            hsend[0, 0, 2] = jnp.broadcast_to(small[1, 0:1], (8, 128))
            hsend[0, 1, 2] = jnp.broadcast_to(small[2, 3:4], (8, 128))
        ready()
        for copy in halo_copies(slot):
            copy.start()

    def inject(cw, ce, sign):
        open_w, open_e = small[1] * sign, small[2] * sign
        first = [open_w * jnp.where(xpos == 0, srl(ce, -p), 0.0) for p in range(PAIRS)]
        last = [open_e * jnp.where(xpos == 3, srl(cw, 3 - p), 0.0) for p in range(PAIRS)]
        return first, last

    def take_halo(slot, sign):
        for copy in halo_copies(slot):
            copy.wait_recv()
        cw, ce = hrecv[slot, 0, 0], hrecv[slot, 1, 0]
        own_w, own_e = hsend[slot, 0, 0], hsend[slot, 1, 0]
        ahead_w = hrecv[slot, 0, 1] + (glow[0] * sign) * (hrecv[0, 0, 2] * own_e)
        ahead_e = hrecv[slot, 1, 1] + (gupp[P_SIZE - 1] * sign) * (hrecv[0, 1, 2] * own_w)
        return inject(cw, ce, sign), inject(ahead_w, ahead_e, -1.0)

    edge_lane = lane == jnp.where(low, 0, 127)

    def yfaces(get):
        own, across = [], []
        for a in range(P_SIZE):
            vs = [get(a, p) for p in range(PAIRS)]
            s = dot((gcoef[p], vs[p]) for p in range(PAIRS))
            t = dot((gcoef[PAIRS + p], vs[p]) for p in range(PAIRS))
            u = halves(s, t) + srl(halves(t, s), 4)
            q = srl(u, 4)
            own.append(u)
            across.append(halves(lrl(q, 1), lrl(q, 127)))
        return own, across

    near = (-1, 0, 1)
    around = [(o, dy) for dy in (-1, 1, 0) for o in near if (o, dy) != (0, 0)]

    def y_copy(o, dy):
        spot = (1 - dy, near.index(-o))
        return pltpu.make_async_remote_copy(
            src_ref=ysend,
            dst_ref=yrecv.at[spot],
            send_sem=ys_sem.at[spot],
            recv_sem=yr_sem.at[spot],
            device_id=at(o, dy),
            device_id_type=MESH,
        )

    def send_yfaces(across):
        packed = across[0]
        for a in range(1, P_SIZE):
            mask = lane == jnp.where(low, a, a - 1)
            packed = jnp.where(mask, lrl(across[a], a), packed)
        ysend[...] = packed
        yrecv[1, 1] = packed
        for o, dy in around:
            y_copy(o, dy).start()

    def apply(get, react, fields, sides, own, across, emit):
        stiff, open_w, open_e, open_y = fields
        for a in range(P_SIZE):
            vs = [get(a, p) for p in range(PAIRS)]
            ss = [srl(v, 4) for v in vs]
            term = own[a] - open_y * across[a]
            for p in range(PAIRS):
                acc = None
                for r in range(PAIRS):
                    k = (p * PAIRS + r) * 2
                    part = coef[k] * vs[r] + coef[k + 1] * ss[r]
                    acc = part if acc is None else acc + part
                other = dot((line[a, c], get(c, p)) for c in range(P_SIZE))
                value = react(a, p) * vs[p] + stiff * (acc + other)
                if p == 0:
                    value = value + jnp.where(low, term, 0.0)
                if p == PAIRS - 1:
                    value = value + jnp.where(low, 0.0, term)
                if (a, p) in sides:
                    value = value + sides[a, p]
                emit(a, p, value)

    def operate(get, faces, given, emit):
        fw, fe = faces
        fields = [small[f] for f in range(4)]
        sides = {}
        for p in range(PAIRS):
            nb_e = jnp.where(xpos == 3, 0.0, srl(fw[p], 7))
            nb_w = jnp.where(xpos == 0, 0.0, srl(fe[p], 1))
            sides[0, p] = fw[p] - fields[1] * nb_w
            sides[P_SIZE - 1, p] = fe[p] - fields[2] * nb_e
        own, across = given or yfaces(get)
        if given:
            across = [jnp.where(edge_lane, 0.0, v) for v in across]
            react = functools.partial(tile, rea)
        else:
            react = lambda a, p: tile(rea, a, p) - shift
        apply(get, react, fields, sides, own, across, emit)

    def gather_rows(accs):
        zero = jnp.zeros((8, 128), jnp.float32)
        level = list(accs) + [zero] * (8 - len(accs))
        for step in (1, 2, 4):
            keep = (sub // step) % 2 == 0
            level = [
                jnp.where(keep, level[i], level[i + 1])
                + srl(jnp.where(keep, level[i + 1], level[i]), step)
                for i in range(0, len(level), 2)
            ]
        return level[0]

    def fold(v):
        for step in (4, 2, 1):
            v = v + srl(v, step)
        return v

    def row_copy(slot, device):
        return pltpu.make_async_remote_copy(
            src_ref=rsend.at[slot],
            dst_ref=rrecv.at[slot, pl.ds(me, 1)],
            send_sem=rs_sem.at[slot],
            recv_sem=rr_sem.at[slot],
            device_id=device,
            device_id_type=MESH,
        )

    def pack_sums(accs, start):
        sums = jnp.sum(gather_rows(accs), axis=1, keepdims=True)
        return jnp.where(lane == sub + start, sums, 0.0)

    def start_reduce(slot, packed):
        row = fold(packed)[0:1]
        rsend[slot] = row
        rrecv[slot, pl.ds(me, 1)] = row
        for_peers(lambda device: row_copy(slot, device).start())

    def end_reduce(slot):
        block = rrecv.at[slot, pl.ds(0, n - 1)]
        pltpu.make_async_copy(block, block, rr_sem.at[slot]).wait()
        value = rrecv[slot, 0:8]
        for g in range(1, n // 8):
            value = value + rrecv[slot, 8 * g:8 * g + 8]
        value = fold(value)
        return lambda k: jnp.broadcast_to(value[:, k:k + 1], (8, 128))

    def narrow_copy(late, o, dy):
        rows = pl.ds(0, PAIRS) if late else pl.ds(PAIRS, PAIRS + 1)
        side, j = (0 if dy > 0 else 1), near.index(-o)
        sems = (1 if late else 0, side, j)
        return pltpu.make_async_remote_copy(
            src_ref=narrow.at[rows],
            dst_ref=narrow_in.at[side, j, rows],
            send_sem=ns_sem.at[sems],
            recv_sem=nr_sem.at[sems],
            device_id=at(o, dy),
            device_id_type=MESH,
        )

    def wide_copy(late, o):
        rows = pl.ds(0, P_SIZE) if late else pl.ds(P_SIZE, P_SIZE + 1)
        j = near.index(-o)
        sems = (1 if late else 0, j)
        return pltpu.make_async_remote_copy(
            src_ref=wide.at[1, rows],
            dst_ref=wide.at[j, rows],
            send_sem=ws_sem.at[sems],
            recv_sem=wr_sem.at[sems],
            device_id=at(o, 0),
            device_id_type=MESH,
        )

    def far_copy(way, o):
        return pltpu.make_async_remote_copy(
            src_ref=far_send.at[way],
            dst_ref=far_in.at[way],
            send_sem=fs_sem.at[way],
            recv_sem=fr_sem.at[way],
            device_id=at(o, 0),
            device_id_type=MESH,
        )

    def strip_copies(late):
        copies = [narrow_copy(late, o, dy) for dy in (-1, 1) for o in near]
        return copies + [wide_copy(late, o) for o in (-1, 1)]

    def far_copies():
        return [far_copy(0, -2), far_copy(1, 2)]

    def pack_wide(items, index):
        parts = []
        for p, v in enumerate(items):
            parts.append((within(32 * p, SLOT), lrl(v, 32 * p)))
            spot = (32 * p + 48) % 128
            parts.append((within(spot, SLOT), lrl(v, spot - (128 - OWNED))))
        wide[1, index] = overlay(parts)

    def pack_narrow(pairs, index):
        parts = []
        for i, items in enumerate(pairs):
            for p, v in enumerate(items):
                spot = SLOT * p + 8 * i
                parts.append((within(spot, 8), lrl(v, spot - (128 - GHOSTS))))
                parts.append((within(64 + spot, 8), lrl(v, 64 + spot)))
        narrow[index] = overlay(parts)

    def pack_field(ref, wide_at, narrow_at):
        rows = [[tile(ref, a, p) for p in range(PAIRS)] for a in range(P_SIZE)]
        for a in range(P_SIZE):
            pack_wide(rows[a], wide_at + a)
        for q in range(PAIRS):
            pack_narrow(rows[2 * q:2 * q + 2], narrow_at + q)

    def pack_small():
        items = [small[f] for f in range(4)]
        pack_wide(items, 2 * P_SIZE)
        pack_narrow([items], 2 * PAIRS)

    def finish_first():
        for dy in (-1, 1):
            y_copy(0, dy).wait_recv()
        cy = halves(yrecv[0, 1], yrecv[2, 1])
        first = bas.at[0]
        for a in range(P_SIZE):
            term = small[3] * jnp.where(edge_lane, lrl(cy, -a), 0.0)
            put(first, a, 0, tile(first, a, 0) + jnp.where(low, term, 0.0))
            last = PAIRS - 1
            put(first, a, last, tile(first, a, last) + jnp.where(low, 0.0, term))
        cw, ce = pack_faces(xfaces(functools.partial(tile, first)))
        far_send[0] = cw
        far_send[1] = ce
        for copy in far_copies():
            copy.start()

    def unpack(wide_at, narrow_at, i, p):
        parts = []
        for j in range(3):
            mask = within(SLOT * (j + 1), OWNED) | within(64 + SLOT * j, OWNED)
            parts.append((mask, lrl(wide[j, wide_at], SLOT * (j + 1) - 32 * p)))
        for j in range(3):
            spot = SLOT * j + OWNED
            both = jnp.where(lane < 64, narrow_in[0, j, narrow_at], narrow_in[1, j, narrow_at])
            mask = within(spot, GHOSTS) | within(64 + spot, GHOSTS)
            parts.append((mask, lrl(both, spot - SLOT * p - 8 * i)))
        return overlay(parts)

    def unpack_early():
        for a, p in tiles():
            value = unpack(P_SIZE + a, PAIRS + a // 2, a % 2, p)
            put(page_rea, a, p, value - shift)
        for f in range(4):
            page_small[f] = unpack(2 * P_SIZE, 2 * PAIRS, 0, f)

    def unpack_late():
        parts, marks = [], None
        for j in range(3):
            for start, lows, upps in (
                (SLOT * (j + 1), yrecv[0, j], yrecv[1, j]),
                (64 + SLOT * j + OWNED, yrecv[1, j], yrecv[2, j]),
            ):
                parts.append((within(start - 1, P_SIZE + 1), lrl(halves(lows, upps), start)))
                mark = lane == jnp.where(low, start, start - 1)
                marks = mark if marks is None else marks | mark
        lines = overlay(parts)
        open_y = jnp.where(marks, page_small[3], 0.0)
        for a in range(P_SIZE):
            term = open_y * lrl(lines, -a)
            for p in range(PAIRS):
                value = unpack(a, a // 2, a % 2, p)
                if p == 0:
                    value = value + jnp.where(low, term, 0.0)
                if p == PAIRS - 1:
                    value = value + jnp.where(low, 0.0, term)
                put(page_a, a, p, value)

    def page_level(level):
        given, out = (page_a, page_b) if level % 2 else (page_b, page_a)
        get = functools.partial(tile, given)
        fields = [page_small[f] for f in range(4)]
        fw, fe = xfaces(get)
        if level == 1:
            cw, ce = far_in[0], far_in[1]
            skip = 128 - OWNED
            east = jnp.where(lane < 64, lrl(cw, 3 * SLOT), lrl(cw, 6 * SLOT - skip))
            west = jnp.where(lane < 64, lrl(ce, SLOT), lrl(ce, 4 * SLOT - skip))
            last = within(2 * SLOT + OWNED, SLOT) | within(6 * SLOT, SLOT)
            first = within(OWNED, SLOT) | within(4 * SLOT, SLOT)
        sides = {}
        for p in range(PAIRS):
            e, w = lrl(srl(fw[p], 3), -SLOT), lrl(srl(fe[p], 5), SLOT)
            if level == 1:
                e = jnp.where(last, srl(east, 3 - p), e)
                w = jnp.where(first, srl(west, -p), w)
            nb_e = jnp.where(xpos == 3, e, srl(fw[p], 7))
            nb_w = jnp.where(xpos == 0, w, srl(fe[p], 1))
            sides[0, p] = fw[p] - fields[1] * nb_w
            sides[P_SIZE - 1, p] = fe[p] - fields[2] * nb_e
        own, across = yfaces(get)

        def emit(a, p, value):
            put(out, a, p, value)
            south = lrl(value, -2 * SLOT)
            north = lrl(value, 128 - OWNED - 5 * SLOT)
            patch[level - 1, a * PAIRS + p] = jnp.where(lane < 64, south, north)

        apply(get, functools.partial(tile, page_rea), fields, sides, own, across, emit)

    edge = (lane < VECS) | (lane >= 128 - VECS)

    def patched(level, a, p, v):
        if level == 0:
            return v
        return jnp.where(edge, patch[level - 1, a * PAIRS + p], v)

    def finish_rows(ref, first, last):
        for p in range(PAIRS):
            put(ref, 0, p, tile(ref, 0, p) + first[p])
            put(ref, P_SIZE - 1, p, tile(ref, P_SIZE - 1, p) + last[p])

    loads[0].wait()
    get = functools.partial(tile, ini)
    faces = xfaces(get)
    given = yfaces(get)
    loads[5].wait()
    loads[6].wait()
    operate(get, faces, given, lambda a, p, v: put(bas.at[0], a, p, tile(src, a, p) - v))

    for step in range(VECS // 2):
        now, after = bas.at[2 * step], bas.at[2 * step + 1]
        fw, fe = xfaces(functools.partial(tile, now))
        if step == 0:
            send_halo(0, faces, (fw, fe), lambda: pl.semaphore_wait(barrier, n - 1))
            send_yfaces(given[1])
            pack_field(rea, P_SIZE, PAIRS)
            pack_small()
            for copy in strip_copies(False):
                copy.start()
        else:
            send_halo(step, faces, (fw, fe))
        if step == 1:
            accs = [None] * 3
            for a, p in tiles():
                u, v = tile(bas.at[0], a, p), tile(bas.at[1], a, p)
                new = [u * u, u * v, v * v]
                accs = new if accs[0] is None else [s + t for s, t in zip(accs, new)]
            start_reduce(0, pack_sums(accs, 0))
        if step == 2:
            finish_first()
            for copy in strip_copies(False):
                copy.wait_recv()
            unpack_early()
        (first, last), extra = take_halo(step, 1.0 if step == 0 else -1.0)
        fw = [fw[p] + glow[0] * first[p] + glow[P_SIZE - 1] * last[p] for p in range(PAIRS)]
        fe = [fe[p] + gupp[0] * first[p] + gupp[P_SIZE - 1] * last[p] for p in range(PAIRS)]
        finish_rows(now, first, last)
        if step == 0:
            pack_field(now, 0, 0)
            for copy in strip_copies(True):
                copy.start()
        operate(functools.partial(tile, now), (fw, fe), None, functools.partial(put, after))
        finish_rows(after, *extra)
        if step < VECS // 2 - 1:
            get = functools.partial(tile, after)
            faces = xfaces(get)
            operate(get, faces, None, functools.partial(put, bas.at[2 * step + 2]))

    for copy in strip_copies(True) + far_copies():
        copy.wait_recv()
    for o, dy in around:
        if o or not dy:
            y_copy(o, dy).wait_recv()
    unpack_late()
    for k in range(1, VECS):
        page_level(k)

    sums = end_reduce(0)
    size = jnp.maximum(sums(0), 1e-30)
    mean = sums(1) / size
    spread = jnp.sqrt(jnp.maximum(sums(2) / size - mean * mean, 0.0)) + 0.1
    inv = 1.0 / spread
    ratio = mean * inv
    theta = shift + mean
    powers = [None, inv]
    for k in range(2, VECS):
        powers.append(powers[k - 1] * inv)

    pairs = [(i, j) for j in range(VECS) for i in range(j + 1)]
    accs = None
    for a, p in tiles():
        lev = []
        for k in range(VECS):
            v = patched(k, a, p, tile(bas.at[k], a, p))
            lev.append(v if k == 0 else v * powers[k])
        vecs = [lev[0]]
        for k in range(1, VECS):
            lev = [lev[i + 1] - ratio * lev[i] for i in range(len(lev) - 1)]
            vecs.append(lev[0])
        for k in range(1, VECS):
            put(bas.at[k], a, p, vecs[k])
        new = [vecs[i] * vecs[j] for i, j in pairs]
        accs = new if accs is None else [s + t for s, t in zip(accs, new)]
    packed = pack_sums(accs[:8], 0) + pack_sums(accs[8:16], 8) + pack_sums(accs[16:], 16)
    start_reduce(1, packed)
    sums = end_reduce(1)

    gram = {}
    for k, (i, j) in enumerate(pairs):
        gram[i, j] = sums(k) * (1.0 / total)
    def times_gram(u, rows):
        return [
            dot((gram[min(i, r), max(i, r)], u[i]) for i in range(len(u))) for r in range(rows)
        ]

    hess = jnp.zeros((8, 128), jnp.float32)
    combos = [[1.0 / jnp.sqrt(gram[0, 0] + FLOOR)]]
    for j in range(ITERS):
        c = combos[j]
        u = [theta * c[0]]
        for i in range(1, j + 1):
            u.append(spread * c[i - 1] + theta * c[i])
        u.append(spread * c[j])
        g = times_gram(u, j + 1)
        rest = list(u)
        for i in range(j + 1):
            h = dot(zip(combos[i], g))
            hess = jnp.where((sub == i) & (lane == j), h, hess)
            for k in range(i + 1):
                rest[k] = rest[k] - h * combos[i][k]
        square = dot(zip(rest, times_gram(rest, j + 2)))
        beta = jnp.sqrt(jnp.maximum(square, 0.0) + FLOOR)
        hess = jnp.where((sub == j + 1) & (lane == j), beta, hess)
        post = 1.0 / beta
        combos.append([r * post for r in rest])

    for a, p in tiles():
        vecs = [tile(bas.at[k], a, p) for k in range(VECS)]
        for j in reversed(range(VECS)):
            put(bas.at[j], a, p, dot(zip(combos[j], vecs)))
    hess_out[...] = hess[0:VECS, 0:ITERS]

    halos = [copy for slot in range(VECS // 2) for copy in halo_copies(slot)]
    edges = strip_copies(False) + strip_copies(True) + far_copies()
    for copy in halos + edges + [y_copy(o, dy) for o, dy in around]:
        copy.wait_send()
    for slot in range(2):
        block = rrecv.at[slot, pl.ds(0, n - 1)]
        pltpu.make_async_copy(block, block, rs_sem.at[slot]).wait()


def store(hess, basis, hess_out, basis_out, sem):
    copies = [
        pltpu.make_async_copy(basis, basis_out, sem.at[0]),
        pltpu.make_async_copy(hess, hess_out, sem.at[1]),
    ]
    for copy in copies:
        copy.start()
    for copy in copies:
        copy.wait()


def body(nx, ny, source, initial, reaction, stiffness, line_op, face_deriv, wall_flags):
    nodes, ex, ey = source.shape
    n = nx * ny
    rows = nodes * ex
    flat = (rows, ey)
    total = float(nodes * ex * nx * ey * ny)
    vmem = pl.BlockSpec(memory_space=pltpu.VMEM)
    hbm = pl.BlockSpec(memory_space=pl.ANY)

    def array(*lead):
        return pltpu.VMEM(lead + (8, 128), jnp.float32)

    dma = pltpu.SemaphoreType.DMA
    hess, basis = pl.pallas_call(
        functools.partial(kernel, nx, ny, total),
        out_shape=(
            pltpu.VMEM((VECS, ITERS), jnp.float32),
            pltpu.VMEM((VECS,) + flat, jnp.float32),
        ),
        in_specs=[hbm] * 7,
        out_specs=(vmem, vmem),
        scratch_shapes=[
            pltpu.SMEM(line_op.shape, jnp.float32),
            pltpu.SMEM(face_deriv.shape, jnp.float32),
            pltpu.VMEM(stiffness.shape, jnp.float32),
            pltpu.VMEM(wall_flags.shape, wall_flags.dtype),
            array(2 * PAIRS * PAIRS),
            array(2 * PAIRS),
            array(4),
            pltpu.VMEM(flat, jnp.float32),
            pltpu.VMEM(flat, jnp.float32),
            pltpu.VMEM(flat, jnp.float32),
            array(3, WIDE),
            array(NARROW),
            array(2, 3, NARROW),
            array(2),
            array(2),
            pltpu.VMEM(flat, jnp.float32),
            array(4),
            pltpu.VMEM(flat, jnp.float32),
            pltpu.VMEM(flat, jnp.float32),
            array(ITERS, P_SIZE * PAIRS),
            dma((7,)),
            array(VECS // 2, 2, 3),
            array(VECS // 2, 2, 3),
            array(),
            array(3, 3),
            pltpu.VMEM((2, 1, 128), jnp.float32),
            pltpu.VMEM((2, n, 128), jnp.float32),
            dma((VECS // 2, 2)),
            dma((VECS // 2, 2)),
            dma((3, 3)),
            dma((3, 3)),
            dma((2, 3)),
            dma((2, 3)),
            dma((2, 2, 3)),
            dma((2, 2, 3)),
            dma((2,)),
            dma((2,)),
            dma((2,)),
            dma((2,)),
        ],
        compiler_params=pltpu.CompilerParams(collective_id=0, has_side_effects=True),
    )(
        line_op, face_deriv, source.reshape(flat), initial.reshape(flat), reaction.reshape(flat),
        stiffness, wall_flags,
    )
    hess = pltpu.with_memory_space_constraint(hess, pltpu.VMEM)
    basis = pltpu.with_memory_space_constraint(basis, pltpu.VMEM)
    hess, basis = pl.pallas_call(
        store,
        out_shape=(
            jax.ShapeDtypeStruct(hess.shape, jnp.float32),
            jax.ShapeDtypeStruct(basis.shape, jnp.float32),
        ),
        in_specs=[hbm, hbm],
        out_specs=(hbm, hbm),
        scratch_shapes=[pltpu.SemaphoreType.DMA((2,))],
    )(hess, basis)
    return hess, basis.reshape((VECS, nodes, ex, ey))


def solution(mesh):
    return jax.shard_map(
        functools.partial(body, mesh.shape["gx"], mesh.shape["gy"]),
        mesh=mesh,
        in_specs=(
            P(None, "gx", "gy"),
            P(None, "gx", "gy"),
            P(None, "gx", "gy"),
            P("gx", "gy"),
            P(),
            P(),
            P(None, "gx", "gy"),
        ),
        out_specs=(P(), P(None, None, "gx", "gy")),
        check_vma=False,
    )
```

```python
import functools

import jax
import jax.numpy as jnp
from jax import lax
from jax.experimental import pallas as pl
from jax.experimental.pallas import tpu as pltpu
from jax.sharding import PartitionSpec as P

P_SIZE = 8
PAIRS = P_SIZE // 2
ITERS = 5
VECS = ITERS + 1
TAU = 2.0
FLOOR = 0.1
SLOT = 16
GHOSTS = ITERS
OWNED = SLOT - GHOSTS
WIDE = 2 * P_SIZE + 1
NARROW = PAIRS + 1
MESH = pl.DeviceIdType.MESH


def kernel(
    nx, ny, total,
    line_any, deriv_any, src_any, ini_any, rea_any, stf_any, wal_any,
    hess_out, bas,
    line, deriv, stf, wal, coef, gcoef, small, src, ini, rea,
    wide, narrow, narrow_in, far_send, far_in,
    page_rea, page_small, page_a, page_b, patch,
    in_sem, hsend, hrecv, ysend, yrecv, rsend, rrecv,
    hs_sem, hr_sem, ys_sem, yr_sem, ws_sem, wr_sem, ns_sem, nr_sem,
    fs_sem, fr_sem, rs_sem, rr_sem,
):
    n = nx * ny
    gx, gy = lax.axis_index("gx"), lax.axis_index("gy")
    me = gx * ny + gy

    side = gy // (ny // 2)
    offsets = sorted(range(1, nx), key=lambda d: abs(2 * d - nx))

    def for_peers(act):
        def column(k, own_column):
            across = side * k + (1 - side) * (ny - 1 - k)
            for d in offsets:
                act((lax.rem(gx + d, nx), across))
            if own_column:
                skip = jnp.where(k >= (side * gy + (1 - side) * (ny - 1 - gy)), 1, 0)
                act((gx, across + (2 * side - 1) * skip))

        if n <= 64:
            for k in range(ny - 1):
                column(k, True)
        else:
            lax.fori_loop(0, ny - 1, lambda k, c: (column(k, True), c)[1], 0)
        column(ny - 1, False)

    def at(dx, dy):
        return (lax.rem(gx + dx + nx, nx), lax.rem(gy + dy + ny, ny))

    barrier = pltpu.get_barrier_semaphore()

    def greet(device):
        pl.semaphore_signal(barrier, inc=1, device_id=device, device_id_type=MESH)

    loads = [
        pltpu.make_async_copy(given, held, in_sem.at[k])
        for k, (given, held) in enumerate((
            (ini_any, ini), (line_any, line), (deriv_any, deriv), (stf_any, stf),
            (wal_any, wal), (src_any, src), (rea_any, rea),
        ))
    ]
    for load in loads:
        load.start()
    for_peers(greet)
    for load in loads[1:5]:
        load.wait()

    sub = lax.broadcasted_iota(jnp.int32, (8, 128), 0)
    lane = lax.broadcasted_iota(jnp.int32, (8, 128), 1)
    low = sub < 4
    xpos = sub % 4
    def srl(v, s):
        s = s % 8
        return v if s == 0 else pltpu.roll(v, s, 0)

    def lrl(v, s):
        s = s % 128
        return v if s == 0 else pltpu.roll(v, s, 1)

    def halves(a, b):
        return jnp.where(low, a, b)

    def within(start, count):
        return (lane >= start) & (lane < start + count)

    def overlay(parts):
        out = None
        for mask, v in parts:
            out = v if out is None else jnp.where(mask, v, out)
        return out

    def dot(pairs):
        out = None
        for c, v in pairs:
            out = c * v if out is None else out + c * v
        return out

    for p in range(PAIRS):
        for r in range(PAIRS):
            k = (p * PAIRS + r) * 2
            coef[k] = halves(line[2 * p, 2 * r], line[2 * p + 1, 2 * r + 1])
            coef[k + 1] = halves(line[2 * p, 2 * r + 1], line[2 * p + 1, 2 * r])
    glow = [0.5 * deriv[c] + (TAU if c == 0 else 0.0) for c in range(P_SIZE)]
    gupp = [
        0.5 * deriv[P_SIZE - 1 - c] + (TAU if c == P_SIZE - 1 else 0.0) for c in range(P_SIZE)
    ]
    for p in range(PAIRS):
        gcoef[p] = halves(glow[2 * p], glow[2 * p + 1])
        gcoef[PAIRS + p] = halves(gupp[2 * p], gupp[2 * p + 1])
    small[0, 0:4] = stf[...]
    small[0, 4:8] = stf[...]
    opened = [1.0 - wal[f].astype(jnp.float32) for f in range(4)]
    for slot, (first, second) in enumerate(((0, 0), (1, 1), (2, 3))):
        small[slot + 1, 0:4] = opened[first]
        small[slot + 1, 4:8] = opened[second]
    trace = line[0, 0]
    for c in range(1, P_SIZE):
        trace = trace + line[c, c]
    shift = 3.0 + 0.25 * trace

    def tile(ref, a, p):
        return ref[pl.ds((a * PAIRS + p) * 8, 8), :]

    def put(ref, a, p, value):
        ref[pl.ds((a * PAIRS + p) * 8, 8), :] = value

    def tiles():
        return [(a, p) for a in range(P_SIZE) for p in range(PAIRS)]

    def xfaces(get):
        fw, fe = [], []
        for p in range(PAIRS):
            vs = [get(c, p) for c in range(P_SIZE)]
            fw.append(dot(zip(glow, vs)))
            fe.append(dot(zip(gupp, vs)))
        return fw, fe

    def halo_copy(slot, way, device):
        rows = pl.ds(0, 3 if slot == 0 else 2)
        return pltpu.make_async_remote_copy(
            src_ref=hsend.at[slot, way, rows],
            dst_ref=hrecv.at[slot, way, rows],
            send_sem=hs_sem.at[slot, way],
            recv_sem=hr_sem.at[slot, way],
            device_id=device,
            device_id_type=MESH,
        )

    def pack_faces(faces):
        fw, fe = faces
        cw, ce = fw[0], srl(fe[0], -3)
        for p in range(1, PAIRS):
            cw = jnp.where(xpos == p, srl(fw[p], p), cw)
            ce = jnp.where(xpos == p, srl(fe[p], p - 3), ce)
        return cw, ce

    def halo_copies(slot):
        return [halo_copy(slot, 0, at(-1, 0)), halo_copy(slot, 1, at(1, 0))]

    def send_halo(slot, faces, ahead, ready=lambda: None):
        for k, pair in enumerate((pack_faces(faces), pack_faces(ahead))):
            for way in range(2):
                hsend[slot, way, k] = pair[way]
        if slot == 0:
            hsend[0, 0, 2] = jnp.broadcast_to(small[1, 0:1], (8, 128))
            hsend[0, 1, 2] = jnp.broadcast_to(small[2, 3:4], (8, 128))
        ready()
        for copy in halo_copies(slot):
            copy.start()

    def inject(cw, ce, sign):
        open_w, open_e = small[1] * sign, small[2] * sign
        first = [open_w * jnp.where(xpos == 0, srl(ce, -p), 0.0) for p in range(PAIRS)]
        last = [open_e * jnp.where(xpos == 3, srl(cw, 3 - p), 0.0) for p in range(PAIRS)]
        return first, last

    def take_halo(slot, sign):
        for copy in halo_copies(slot):
            copy.wait_recv()
        cw, ce = hrecv[slot, 0, 0], hrecv[slot, 1, 0]
        own_w, own_e = hsend[slot, 0, 0], hsend[slot, 1, 0]
        ahead_w = hrecv[slot, 0, 1] + (glow[0] * sign) * (hrecv[0, 0, 2] * own_e)
        ahead_e = hrecv[slot, 1, 1] + (gupp[P_SIZE - 1] * sign) * (hrecv[0, 1, 2] * own_w)
        return inject(cw, ce, sign), inject(ahead_w, ahead_e, -1.0)

    edge_lane = lane == jnp.where(low, 0, 127)

    def yfaces(get):
        own, across = [], []
        for a in range(P_SIZE):
            vs = [get(a, p) for p in range(PAIRS)]
            s = dot((gcoef[p], vs[p]) for p in range(PAIRS))
            t = dot((gcoef[PAIRS + p], vs[p]) for p in range(PAIRS))
            u = halves(s, t) + srl(halves(t, s), 4)
            q = srl(u, 4)
            own.append(u)
            across.append(halves(lrl(q, 1), lrl(q, 127)))
        return own, across

    def y_copy(target, device):
        return pltpu.make_async_remote_copy(
            src_ref=ysend,
            dst_ref=yrecv.at[target],
            send_sem=ys_sem.at[target],
            recv_sem=yr_sem.at[target],
            device_id=device,
            device_id_type=MESH,
        )

    def y_copies():
        return [y_copy(0, at(0, 1)), y_copy(1, at(0, -1))]

    def send_yfaces(across):
        packed = across[0]
        for a in range(1, P_SIZE):
            mask = lane == jnp.where(low, a, a - 1)
            packed = jnp.where(mask, lrl(across[a], a), packed)
        ysend[...] = packed
        for copy in y_copies():
            copy.start()

    def apply(get, react, fields, sides, own, across, emit):
        stiff, open_w, open_e, open_y = fields
        for a in range(P_SIZE):
            vs = [get(a, p) for p in range(PAIRS)]
            ss = [srl(v, 4) for v in vs]
            term = own[a] - open_y * across[a]
            for p in range(PAIRS):
                acc = None
                for r in range(PAIRS):
                    k = (p * PAIRS + r) * 2
                    part = coef[k] * vs[r] + coef[k + 1] * ss[r]
                    acc = part if acc is None else acc + part
                other = dot((line[a, c], get(c, p)) for c in range(P_SIZE))
                value = react(a, p) * vs[p] + stiff * (acc + other)
                if p == 0:
                    value = value + jnp.where(low, term, 0.0)
                if p == PAIRS - 1:
                    value = value + jnp.where(low, 0.0, term)
                if (a, p) in sides:
                    value = value + sides[a, p]
                emit(a, p, value)

    def operate(get, faces, given, emit):
        fw, fe = faces
        fields = [small[f] for f in range(4)]
        sides = {}
        for p in range(PAIRS):
            nb_e = jnp.where(xpos == 3, 0.0, srl(fw[p], 7))
            nb_w = jnp.where(xpos == 0, 0.0, srl(fe[p], 1))
            sides[0, p] = fw[p] - fields[1] * nb_w
            sides[P_SIZE - 1, p] = fe[p] - fields[2] * nb_e
        own, across = given or yfaces(get)
        if given:
            across = [jnp.where(edge_lane, 0.0, v) for v in across]
            react = functools.partial(tile, rea)
        else:
            react = lambda a, p: tile(rea, a, p) - shift
        apply(get, react, fields, sides, own, across, emit)

    def gather_rows(accs):
        zero = jnp.zeros((8, 128), jnp.float32)
        level = list(accs) + [zero] * (8 - len(accs))
        for step in (1, 2, 4):
            keep = (sub // step) % 2 == 0
            level = [
                jnp.where(keep, level[i], level[i + 1])
                + srl(jnp.where(keep, level[i + 1], level[i]), step)
                for i in range(0, len(level), 2)
            ]
        return level[0]

    def fold(v):
        for step in (4, 2, 1):
            v = v + srl(v, step)
        return v

    def row_copy(slot, device):
        return pltpu.make_async_remote_copy(
            src_ref=rsend.at[slot],
            dst_ref=rrecv.at[slot, pl.ds(me, 1)],
            send_sem=rs_sem.at[slot],
            recv_sem=rr_sem.at[slot],
            device_id=device,
            device_id_type=MESH,
        )

    def pack_sums(accs, start):
        sums = jnp.sum(gather_rows(accs), axis=1, keepdims=True)
        return jnp.where(lane == sub + start, sums, 0.0)

    def start_reduce(slot, packed):
        row = fold(packed)[0:1]
        rsend[slot] = row
        rrecv[slot, pl.ds(me, 1)] = row
        for_peers(lambda device: row_copy(slot, device).start())

    def end_reduce(slot):
        block = rrecv.at[slot, pl.ds(0, n - 1)]
        pltpu.make_async_copy(block, block, rr_sem.at[slot]).wait()
        value = rrecv[slot, 0:8]
        for g in range(1, n // 8):
            value = value + rrecv[slot, 8 * g:8 * g + 8]
        value = fold(value)
        return lambda k: jnp.broadcast_to(value[:, k:k + 1], (8, 128))

    near = (-1, 0, 1)

    def narrow_copy(late, o, dy):
        rows = pl.ds(0, 2) if late else pl.ds(2, 3)
        side, j = (0 if dy > 0 else 1), near.index(-o)
        sems = (1 if late else 0, side, j)
        return pltpu.make_async_remote_copy(
            src_ref=narrow.at[side, rows],
            dst_ref=narrow_in.at[side, j, rows],
            send_sem=ns_sem.at[sems],
            recv_sem=nr_sem.at[sems],
            device_id=at(o, dy),
            device_id_type=MESH,
        )

    def wide_copy(late, o):
        rows = pl.ds(0, P_SIZE) if late else pl.ds(P_SIZE, P_SIZE + 1)
        j = near.index(-o)
        sems = (1 if late else 0, j)
        return pltpu.make_async_remote_copy(
            src_ref=wide.at[1, rows],
            dst_ref=wide.at[j, rows],
            send_sem=ws_sem.at[sems],
            recv_sem=wr_sem.at[sems],
            device_id=at(o, 0),
            device_id_type=MESH,
        )

    def far_copy(way, o):
        return pltpu.make_async_remote_copy(
            src_ref=far_send.at[way],
            dst_ref=far_in.at[way],
            send_sem=fs_sem.at[way],
            recv_sem=fr_sem.at[way],
            device_id=at(o, 0),
            device_id_type=MESH,
        )

    def strip_copies(late):
        copies = [narrow_copy(late, o, dy) for dy in (-1, 1) for o in near]
        copies += [wide_copy(late, o) for o in (-1, 1)]
        if late:
            copies += [far_copy(0, -2), far_copy(1, 2)]
        return copies

    def pack_wide(items, index):
        parts = []
        for p, v in enumerate(items):
            parts.append((within(32 * p, SLOT), lrl(v, 32 * p)))
            spot = (32 * p + 48) % 128
            parts.append((within(spot, SLOT), lrl(v, spot - (128 - OWNED))))
        wide[1, index] = overlay(parts)

    def pack_narrow(rows, index):
        upps, lows = [], []
        for i, items in enumerate(rows):
            for p, v in enumerate(items):
                spot = 32 * p + 8 * i
                upps.append((within(spot, 8), lrl(v, spot - (128 - GHOSTS))))
                lows.append((within(spot, 8), lrl(v, spot)))
        narrow[0, index] = overlay(upps)
        narrow[1, index] = overlay(lows)

    def pack_field(ref, wide_at, narrow_at):
        rows = [[tile(ref, a, p) for p in range(PAIRS)] for a in range(P_SIZE)]
        for a in range(P_SIZE):
            pack_wide(rows[a], wide_at + a)
        for q in range(2):
            pack_narrow(rows[4 * q:4 * q + 4], narrow_at + q)

    def pack_small():
        items = [small[f] for f in range(4)]
        pack_wide(items, 2 * P_SIZE)
        pack_narrow([items], PAIRS)

    def finish_first():
        for copy in y_copies():
            copy.wait_recv()
        cy = halves(yrecv[0], yrecv[1])
        first = bas.at[0]
        for a in range(P_SIZE):
            term = small[3] * jnp.where(edge_lane, lrl(cy, -a), 0.0)
            put(first, a, 0, tile(first, a, 0) + jnp.where(low, term, 0.0))
            last = PAIRS - 1
            put(first, a, last, tile(first, a, last) + jnp.where(low, 0.0, term))
        cw, ce = pack_faces(xfaces(functools.partial(tile, first)))
        far_send[0] = cw
        far_send[1] = ce
        pack_field(first, 0, 0)
        for copy in strip_copies(True):
            copy.start()

    def unpack(wide_at, narrow_at, i, p):
        parts = []
        for j in range(3):
            mask = within(SLOT * (j + 1), OWNED) | within(64 + SLOT * j, OWNED)
            parts.append((mask, lrl(wide[j, wide_at], SLOT * (j + 1) - 32 * p)))
        for j in range(3):
            for side in range(2):
                spot = 64 * side + SLOT * j + OWNED
                v = lrl(narrow_in[side, j, narrow_at], spot - 32 * p - 8 * i)
                parts.append((within(spot, GHOSTS), v))
        return overlay(parts)

    def unpack_early():
        for a, p in tiles():
            value = unpack(P_SIZE + a, 2 + a // 4, a % 4, p)
            put(page_rea, a, p, value - shift)
        for f in range(4):
            page_small[f] = unpack(2 * P_SIZE, PAIRS, 0, f)

    def unpack_late():
        for a, p in tiles():
            put(page_a, a, p, unpack(a, a // 4, a % 4, p))

    def page_level(level):
        given, out = (page_a, page_b) if level % 2 else (page_b, page_a)
        get = functools.partial(tile, given)
        fields = [page_small[f] for f in range(4)]
        fw, fe = xfaces(get)
        if level == 1:
            cw, ce = far_in[0], far_in[1]
            skip = 128 - OWNED
            east = jnp.where(lane < 64, lrl(cw, 3 * SLOT), lrl(cw, 6 * SLOT - skip))
            west = jnp.where(lane < 64, lrl(ce, SLOT), lrl(ce, 4 * SLOT - skip))
            last = within(2 * SLOT + OWNED, SLOT) | within(6 * SLOT, SLOT)
            first = within(OWNED, SLOT) | within(4 * SLOT, SLOT)
        sides = {}
        for p in range(PAIRS):
            e, w = lrl(srl(fw[p], 3), -SLOT), lrl(srl(fe[p], 5), SLOT)
            if level == 1:
                e = jnp.where(last, srl(east, 3 - p), e)
                w = jnp.where(first, srl(west, -p), w)
            nb_e = jnp.where(xpos == 3, e, srl(fw[p], 7))
            nb_w = jnp.where(xpos == 0, w, srl(fe[p], 1))
            sides[0, p] = fw[p] - fields[1] * nb_w
            sides[P_SIZE - 1, p] = fe[p] - fields[2] * nb_e
        own, across = yfaces(get)

        def emit(a, p, value):
            put(out, a, p, value)
            south = lrl(value, -2 * SLOT)
            north = lrl(value, 128 - OWNED - 5 * SLOT)
            patch[level - 1, a * PAIRS + p] = jnp.where(lane < 64, south, north)

        apply(get, functools.partial(tile, page_rea), fields, sides, own, across, emit)

    edge = (lane < VECS) | (lane >= 128 - VECS)

    def patched(level, a, p, v):
        if level == 0:
            return v
        return jnp.where(edge, patch[level - 1, a * PAIRS + p], v)

    def finish_rows(ref, first, last):
        for p in range(PAIRS):
            put(ref, 0, p, tile(ref, 0, p) + first[p])
            put(ref, P_SIZE - 1, p, tile(ref, P_SIZE - 1, p) + last[p])

    loads[0].wait()
    get = functools.partial(tile, ini)
    faces = xfaces(get)
    given = yfaces(get)
    loads[5].wait()
    loads[6].wait()
    operate(get, faces, given, lambda a, p, v: put(bas.at[0], a, p, tile(src, a, p) - v))

    late = gy == ny - 1
    for step in range(VECS // 2):
        now, after = bas.at[2 * step], bas.at[2 * step + 1]
        fw, fe = xfaces(functools.partial(tile, now))
        if step == 0:
            send_halo(0, faces, (fw, fe), lambda: pl.semaphore_wait(barrier, n - 1))
            send_yfaces(given[1])
            pack_field(rea, P_SIZE, 2)
            pack_small()
            for copy in strip_copies(False):
                copy.start()
        else:
            send_halo(step, faces, (fw, fe))
        if step == 1:
            pl.when(jnp.logical_not(late))(finish_first)
            accs = [None] * 3
            for a, p in tiles():
                u, v = tile(bas.at[0], a, p), tile(bas.at[1], a, p)
                new = [u * u, u * v, v * v]
                accs = new if accs[0] is None else [s + t for s, t in zip(accs, new)]
            start_reduce(0, pack_sums(accs, 0))
        if step == 2:
            pl.when(late)(finish_first)
            for copy in strip_copies(False):
                copy.wait_recv()
            unpack_early()
        (first, last), extra = take_halo(step, 1.0 if step == 0 else -1.0)
        fw = [fw[p] + glow[0] * first[p] + glow[P_SIZE - 1] * last[p] for p in range(PAIRS)]
        fe = [fe[p] + gupp[0] * first[p] + gupp[P_SIZE - 1] * last[p] for p in range(PAIRS)]
        finish_rows(now, first, last)
        operate(functools.partial(tile, now), (fw, fe), None, functools.partial(put, after))
        finish_rows(after, *extra)
        if step < VECS // 2 - 1:
            get = functools.partial(tile, after)
            faces = xfaces(get)
            operate(get, faces, None, functools.partial(put, bas.at[2 * step + 2]))

    for copy in strip_copies(True):
        copy.wait_recv()
    unpack_late()
    for k in range(1, VECS):
        page_level(k)

    sums = end_reduce(0)
    size = jnp.maximum(sums(0), 1e-30)
    mean = sums(1) / size
    spread = jnp.sqrt(jnp.maximum(sums(2) / size - mean * mean, 0.0)) + 0.1
    inv = 1.0 / spread
    ratio = mean * inv
    theta = shift + mean
    powers = [None, inv]
    for k in range(2, VECS):
        powers.append(powers[k - 1] * inv)

    pairs = [(i, j) for j in range(VECS) for i in range(j + 1)]
    accs = None
    for a, p in tiles():
        lev = []
        for k in range(VECS):
            v = patched(k, a, p, tile(bas.at[k], a, p))
            lev.append(v if k == 0 else v * powers[k])
        vecs = [lev[0]]
        for k in range(1, VECS):
            lev = [lev[i + 1] - ratio * lev[i] for i in range(len(lev) - 1)]
            vecs.append(lev[0])
        for k in range(1, VECS):
            put(bas.at[k], a, p, vecs[k])
        new = [vecs[i] * vecs[j] for i, j in pairs]
        accs = new if accs is None else [s + t for s, t in zip(accs, new)]
    packed = pack_sums(accs[:8], 0) + pack_sums(accs[8:16], 8) + pack_sums(accs[16:], 16)
    start_reduce(1, packed)
    sums = end_reduce(1)

    gram = {}
    for k, (i, j) in enumerate(pairs):
        gram[i, j] = sums(k) * (1.0 / total)
    def times_gram(u, rows):
        return [
            dot((gram[min(i, r), max(i, r)], u[i]) for i in range(len(u))) for r in range(rows)
        ]

    hess = jnp.zeros((8, 128), jnp.float32)
    combos = [[1.0 / jnp.sqrt(gram[0, 0] + FLOOR)]]
    for j in range(ITERS):
        c = combos[j]
        u = [theta * c[0]]
        for i in range(1, j + 1):
            u.append(spread * c[i - 1] + theta * c[i])
        u.append(spread * c[j])
        g = times_gram(u, j + 1)
        rest = list(u)
        for i in range(j + 1):
            h = dot(zip(combos[i], g))
            hess = jnp.where((sub == i) & (lane == j), h, hess)
            for k in range(i + 1):
                rest[k] = rest[k] - h * combos[i][k]
        square = dot(zip(rest, times_gram(rest, j + 2)))
        beta = jnp.sqrt(jnp.maximum(square, 0.0) + FLOOR)
        hess = jnp.where((sub == j + 1) & (lane == j), beta, hess)
        post = 1.0 / beta
        combos.append([r * post for r in rest])

    for a, p in tiles():
        vecs = [tile(bas.at[k], a, p) for k in range(VECS)]
        for j in reversed(range(VECS)):
            put(bas.at[j], a, p, dot(zip(combos[j], vecs)))
    hess_out[...] = hess[0:VECS, 0:ITERS]

    halos = [copy for slot in range(VECS // 2) for copy in halo_copies(slot)]
    for copy in halos + y_copies() + strip_copies(False) + strip_copies(True):
        copy.wait_send()
    for slot in range(2):
        block = rrecv.at[slot, pl.ds(0, n - 1)]
        pltpu.make_async_copy(block, block, rs_sem.at[slot]).wait()


def store(hess, basis, hess_out, basis_out, sem):
    copies = [
        pltpu.make_async_copy(basis, basis_out, sem.at[0]),
        pltpu.make_async_copy(hess, hess_out, sem.at[1]),
    ]
    for copy in copies:
        copy.start()
    for copy in copies:
        copy.wait()


def body(nx, ny, source, initial, reaction, stiffness, line_op, face_deriv, wall_flags):
    nodes, ex, ey = source.shape
    n = nx * ny
    rows = nodes * ex
    flat = (rows, ey)
    total = float(nodes * ex * nx * ey * ny)
    vmem = pl.BlockSpec(memory_space=pltpu.VMEM)
    hbm = pl.BlockSpec(memory_space=pl.ANY)

    def array(*lead):
        return pltpu.VMEM(lead + (8, 128), jnp.float32)

    dma = pltpu.SemaphoreType.DMA
    hess, basis = pl.pallas_call(
        functools.partial(kernel, nx, ny, total),
        out_shape=(
            pltpu.VMEM((VECS, ITERS), jnp.float32),
            pltpu.VMEM((VECS,) + flat, jnp.float32),
        ),
        in_specs=[hbm] * 7,
        out_specs=(vmem, vmem),
        scratch_shapes=[
            pltpu.SMEM(line_op.shape, jnp.float32),
            pltpu.SMEM(face_deriv.shape, jnp.float32),
            pltpu.VMEM(stiffness.shape, jnp.float32),
            pltpu.VMEM(wall_flags.shape, wall_flags.dtype),
            array(2 * PAIRS * PAIRS),
            array(2 * PAIRS),
            array(4),
            pltpu.VMEM(flat, jnp.float32),
            pltpu.VMEM(flat, jnp.float32),
            pltpu.VMEM(flat, jnp.float32),
            array(3, WIDE),
            array(2, NARROW),
            array(2, 3, NARROW),
            array(2),
            array(2),
            pltpu.VMEM(flat, jnp.float32),
            array(4),
            pltpu.VMEM(flat, jnp.float32),
            pltpu.VMEM(flat, jnp.float32),
            array(ITERS, P_SIZE * PAIRS),
            dma((7,)),
            array(VECS // 2, 2, 3),
            array(VECS // 2, 2, 3),
            array(),
            array(2),
            pltpu.VMEM((2, 1, 128), jnp.float32),
            pltpu.VMEM((2, n, 128), jnp.float32),
            dma((VECS // 2, 2)),
            dma((VECS // 2, 2)),
            dma((2,)),
            dma((2,)),
            dma((2, 3)),
            dma((2, 3)),
            dma((2, 2, 3)),
            dma((2, 2, 3)),
            dma((2,)),
            dma((2,)),
            dma((2,)),
            dma((2,)),
        ],
        compiler_params=pltpu.CompilerParams(collective_id=0, has_side_effects=True),
    )(
        line_op, face_deriv, source.reshape(flat), initial.reshape(flat), reaction.reshape(flat),
        stiffness, wall_flags,
    )
    hess = pltpu.with_memory_space_constraint(hess, pltpu.VMEM)
    basis = pltpu.with_memory_space_constraint(basis, pltpu.VMEM)
    hess, basis = pl.pallas_call(
        store,
        out_shape=(
            jax.ShapeDtypeStruct(hess.shape, jnp.float32),
            jax.ShapeDtypeStruct(basis.shape, jnp.float32),
        ),
        in_specs=[hbm, hbm],
        out_specs=(hbm, hbm),
        scratch_shapes=[pltpu.SemaphoreType.DMA((2,))],
    )(hess, basis)
    return hess, basis.reshape((VECS, nodes, ex, ey))


def solution(mesh):
    return jax.shard_map(
        functools.partial(body, mesh.shape["gx"], mesh.shape["gy"]),
        mesh=mesh,
        in_specs=(
            P(None, "gx", "gy"),
            P(None, "gx", "gy"),
            P(None, "gx", "gy"),
            P("gx", "gy"),
            P(),
            P(),
            P(None, "gx", "gy"),
        ),
        out_specs=(P(), P(None, None, "gx", "gy")),
        check_vma=False,
    )
```

```python
import functools

import jax
import jax.numpy as jnp
from jax import lax
from jax.experimental import pallas as pl
from jax.experimental.pallas import tpu as pltpu
from jax.sharding import PartitionSpec as P

P_SIZE = 8
PAIRS = P_SIZE // 2
ITERS = 5
VECS = ITERS + 1
TAU = 2.0
FLOOR = 0.1
SLOT = 16
GHOSTS = ITERS
OWNED = SLOT - GHOSTS
WIDE = 2 * P_SIZE + 1
NARROW = PAIRS + 1
MESH = pl.DeviceIdType.MESH


def kernel(
    nx, ny, total,
    line_any, deriv_any, src_any, ini_any, rea_any, stf_any, wal_any,
    hess_out, bas,
    line, deriv, stf, wal, coef, gcoef, small, src, ini, rea,
    wide, narrow, narrow_in, far_send, far_in,
    page_rea, page_small, page_a, page_b, patch,
    in_sem, hsend, hrecv, ysend, yrecv, rsend, rrecv,
    hs_sem, hr_sem, ys_sem, yr_sem, ws_sem, wr_sem, ns_sem, nr_sem,
    fs_sem, fr_sem, rs_sem, rr_sem,
):
    n = nx * ny
    gx, gy = lax.axis_index("gx"), lax.axis_index("gy")
    me = gx * ny + gy

    side = gy // (ny // 2)
    offsets = sorted(range(1, nx), key=lambda d: abs(2 * d - nx))

    def for_peers(act):
        def column(k, own_column):
            across = side * k + (1 - side) * (ny - 1 - k)
            for d in offsets:
                act((lax.rem(gx + d, nx), across))
            if own_column:
                skip = jnp.where(k >= (side * gy + (1 - side) * (ny - 1 - gy)), 1, 0)
                act((gx, across + (2 * side - 1) * skip))

        if n <= 64:
            for k in range(ny - 1):
                column(k, True)
        else:
            lax.fori_loop(0, ny - 1, lambda k, c: (column(k, True), c)[1], 0)
        column(ny - 1, False)

    def at(dx, dy):
        return (lax.rem(gx + dx + nx, nx), lax.rem(gy + dy + ny, ny))

    barrier = pltpu.get_barrier_semaphore()

    def greet(device):
        pl.semaphore_signal(barrier, inc=1, device_id=device, device_id_type=MESH)

    loads = [
        pltpu.make_async_copy(given, held, in_sem.at[k])
        for k, (given, held) in enumerate((
            (ini_any, ini), (line_any, line), (deriv_any, deriv), (stf_any, stf),
            (wal_any, wal), (src_any, src), (rea_any, rea),
        ))
    ]
    for load in loads:
        load.start()
    for_peers(greet)
    for load in loads[1:5]:
        load.wait()

    sub = lax.broadcasted_iota(jnp.int32, (8, 128), 0)
    lane = lax.broadcasted_iota(jnp.int32, (8, 128), 1)
    low = sub < 4
    xpos = sub % 4
    def srl(v, s):
        s = s % 8
        return v if s == 0 else pltpu.roll(v, s, 0)

    def lrl(v, s):
        s = s % 128
        return v if s == 0 else pltpu.roll(v, s, 1)

    def halves(a, b):
        return jnp.where(low, a, b)

    def within(start, count):
        return (lane >= start) & (lane < start + count)

    def overlay(parts):
        out = None
        for mask, v in parts:
            out = v if out is None else jnp.where(mask, v, out)
        return out

    def dot(pairs):
        out = None
        for c, v in pairs:
            out = c * v if out is None else out + c * v
        return out

    for p in range(PAIRS):
        for r in range(PAIRS):
            k = (p * PAIRS + r) * 2
            coef[k] = halves(line[2 * p, 2 * r], line[2 * p + 1, 2 * r + 1])
            coef[k + 1] = halves(line[2 * p, 2 * r + 1], line[2 * p + 1, 2 * r])
    glow = [0.5 * deriv[c] + (TAU if c == 0 else 0.0) for c in range(P_SIZE)]
    gupp = [
        0.5 * deriv[P_SIZE - 1 - c] + (TAU if c == P_SIZE - 1 else 0.0) for c in range(P_SIZE)
    ]
    for p in range(PAIRS):
        gcoef[p] = halves(glow[2 * p], glow[2 * p + 1])
        gcoef[PAIRS + p] = halves(gupp[2 * p], gupp[2 * p + 1])
    small[0, 0:4] = stf[...]
    small[0, 4:8] = stf[...]
    opened = [1.0 - wal[f].astype(jnp.float32) for f in range(4)]
    for slot, (first, second) in enumerate(((0, 0), (1, 1), (2, 3))):
        small[slot + 1, 0:4] = opened[first]
        small[slot + 1, 4:8] = opened[second]
    trace = line[0, 0]
    for c in range(1, P_SIZE):
        trace = trace + line[c, c]
    shift = 3.0 + 0.25 * trace

    def tile(ref, a, p):
        return ref[pl.ds((a * PAIRS + p) * 8, 8), :]

    def put(ref, a, p, value):
        ref[pl.ds((a * PAIRS + p) * 8, 8), :] = value

    def tiles():
        return [(a, p) for a in range(P_SIZE) for p in range(PAIRS)]

    def xfaces(get):
        fw, fe = [], []
        for p in range(PAIRS):
            vs = [get(c, p) for c in range(P_SIZE)]
            fw.append(dot(zip(glow, vs)))
            fe.append(dot(zip(gupp, vs)))
        return fw, fe

    def halo_copy(slot, way, device):
        rows = pl.ds(0, 3 if slot == 0 else 2)
        return pltpu.make_async_remote_copy(
            src_ref=hsend.at[slot, way, rows],
            dst_ref=hrecv.at[slot, way, rows],
            send_sem=hs_sem.at[slot, way],
            recv_sem=hr_sem.at[slot, way],
            device_id=device,
            device_id_type=MESH,
        )

    def pack_faces(faces):
        fw, fe = faces
        cw, ce = fw[0], srl(fe[0], -3)
        for p in range(1, PAIRS):
            cw = jnp.where(xpos == p, srl(fw[p], p), cw)
            ce = jnp.where(xpos == p, srl(fe[p], p - 3), ce)
        return cw, ce

    def halo_copies(slot):
        return [halo_copy(slot, 0, at(-1, 0)), halo_copy(slot, 1, at(1, 0))]

    def send_halo(slot, faces, ahead, ready=lambda: None):
        for k, pair in enumerate((pack_faces(faces), pack_faces(ahead))):
            for way in range(2):
                hsend[slot, way, k] = pair[way]
        if slot == 0:
            hsend[0, 0, 2] = jnp.broadcast_to(small[1, 0:1], (8, 128))
            hsend[0, 1, 2] = jnp.broadcast_to(small[2, 3:4], (8, 128))
        ready()
        for copy in halo_copies(slot):
            copy.start()

    def inject(cw, ce, sign):
        open_w, open_e = small[1] * sign, small[2] * sign
        first = [open_w * jnp.where(xpos == 0, srl(ce, -p), 0.0) for p in range(PAIRS)]
        last = [open_e * jnp.where(xpos == 3, srl(cw, 3 - p), 0.0) for p in range(PAIRS)]
        return first, last

    def take_halo(slot, sign):
        for copy in halo_copies(slot):
            copy.wait_recv()
        cw, ce = hrecv[slot, 0, 0], hrecv[slot, 1, 0]
        own_w, own_e = hsend[slot, 0, 0], hsend[slot, 1, 0]
        ahead_w = hrecv[slot, 0, 1] + (glow[0] * sign) * (hrecv[0, 0, 2] * own_e)
        ahead_e = hrecv[slot, 1, 1] + (gupp[P_SIZE - 1] * sign) * (hrecv[0, 1, 2] * own_w)
        return inject(cw, ce, sign), inject(ahead_w, ahead_e, -1.0)

    edge_lane = lane == jnp.where(low, 0, 127)

    def yfaces(get):
        own, across = [], []
        for a in range(P_SIZE):
            vs = [get(a, p) for p in range(PAIRS)]
            s = dot((gcoef[p], vs[p]) for p in range(PAIRS))
            t = dot((gcoef[PAIRS + p], vs[p]) for p in range(PAIRS))
            u = halves(s, t) + srl(halves(t, s), 4)
            q = srl(u, 4)
            own.append(u)
            across.append(halves(lrl(q, 1), lrl(q, 127)))
        return own, across

    def y_copy(target, device):
        return pltpu.make_async_remote_copy(
            src_ref=ysend,
            dst_ref=yrecv.at[target],
            send_sem=ys_sem.at[target],
            recv_sem=yr_sem.at[target],
            device_id=device,
            device_id_type=MESH,
        )

    def y_copies():
        return [y_copy(0, at(0, 1)), y_copy(1, at(0, -1))]

    def send_yfaces(across):
        packed = across[0]
        for a in range(1, P_SIZE):
            mask = lane == jnp.where(low, a, a - 1)
            packed = jnp.where(mask, lrl(across[a], a), packed)
        ysend[...] = packed
        for copy in y_copies():
            copy.start()

    def apply(get, react, fields, sides, own, across, emit):
        stiff, open_w, open_e, open_y = fields
        for a in range(P_SIZE):
            vs = [get(a, p) for p in range(PAIRS)]
            ss = [srl(v, 4) for v in vs]
            term = own[a] - open_y * across[a]
            for p in range(PAIRS):
                acc = None
                for r in range(PAIRS):
                    k = (p * PAIRS + r) * 2
                    part = coef[k] * vs[r] + coef[k + 1] * ss[r]
                    acc = part if acc is None else acc + part
                other = dot((line[a, c], get(c, p)) for c in range(P_SIZE))
                value = react(a, p) * vs[p] + stiff * (acc + other)
                if p == 0:
                    value = value + jnp.where(low, term, 0.0)
                if p == PAIRS - 1:
                    value = value + jnp.where(low, 0.0, term)
                if (a, p) in sides:
                    value = value + sides[a, p]
                emit(a, p, value)

    def operate(get, faces, given, emit):
        fw, fe = faces
        fields = [small[f] for f in range(4)]
        sides = {}
        for p in range(PAIRS):
            nb_e = jnp.where(xpos == 3, 0.0, srl(fw[p], 7))
            nb_w = jnp.where(xpos == 0, 0.0, srl(fe[p], 1))
            sides[0, p] = fw[p] - fields[1] * nb_w
            sides[P_SIZE - 1, p] = fe[p] - fields[2] * nb_e
        own, across = given or yfaces(get)
        if given:
            across = [jnp.where(edge_lane, 0.0, v) for v in across]
            react = functools.partial(tile, rea)
        else:
            react = lambda a, p: tile(rea, a, p) - shift
        apply(get, react, fields, sides, own, across, emit)

    def gather_rows(accs):
        zero = jnp.zeros((8, 128), jnp.float32)
        level = list(accs) + [zero] * (8 - len(accs))
        for step in (1, 2, 4):
            keep = (sub // step) % 2 == 0
            level = [
                jnp.where(keep, level[i], level[i + 1])
                + srl(jnp.where(keep, level[i + 1], level[i]), step)
                for i in range(0, len(level), 2)
            ]
        return level[0]

    def fold(v):
        for step in (4, 2, 1):
            v = v + srl(v, step)
        return v

    def row_copy(slot, device):
        return pltpu.make_async_remote_copy(
            src_ref=rsend.at[slot],
            dst_ref=rrecv.at[slot, pl.ds(me, 1)],
            send_sem=rs_sem.at[slot],
            recv_sem=rr_sem.at[slot],
            device_id=device,
            device_id_type=MESH,
        )

    def pack_sums(accs, start):
        sums = jnp.sum(gather_rows(accs), axis=1, keepdims=True)
        return jnp.where(lane == sub + start, sums, 0.0)

    def start_reduce(slot, packed):
        row = fold(packed)[0:1]
        rsend[slot] = row
        rrecv[slot, pl.ds(me, 1)] = row
        for_peers(lambda device: row_copy(slot, device).start())

    def end_reduce(slot):
        block = rrecv.at[slot, pl.ds(0, n - 1)]
        pltpu.make_async_copy(block, block, rr_sem.at[slot]).wait()
        value = rrecv[slot, 0:8]
        for g in range(1, n // 8):
            value = value + rrecv[slot, 8 * g:8 * g + 8]
        value = fold(value)
        return lambda k: jnp.broadcast_to(value[:, k:k + 1], (8, 128))

    near = (-1, 0, 1)

    def narrow_copy(late, o, dy):
        rows = pl.ds(0, 2) if late else pl.ds(2, 3)
        side, j = (0 if dy > 0 else 1), near.index(-o)
        sems = (1 if late else 0, side, j)
        return pltpu.make_async_remote_copy(
            src_ref=narrow.at[side, rows],
            dst_ref=narrow_in.at[side, j, rows],
            send_sem=ns_sem.at[0],
            recv_sem=nr_sem.at[sems],
            device_id=at(o, dy),
            device_id_type=MESH,
        )

    def wide_copy(late, o):
        rows = pl.ds(0, P_SIZE) if late else pl.ds(P_SIZE, P_SIZE + 1)
        j = near.index(-o)
        sems = (1 if late else 0, j)
        return pltpu.make_async_remote_copy(
            src_ref=wide.at[1, rows],
            dst_ref=wide.at[j, rows],
            send_sem=ws_sem.at[0],
            recv_sem=wr_sem.at[sems],
            device_id=at(o, 0),
            device_id_type=MESH,
        )

    def far_copy(way, o):
        return pltpu.make_async_remote_copy(
            src_ref=far_send.at[way],
            dst_ref=far_in.at[way],
            send_sem=fs_sem.at[way],
            recv_sem=fr_sem.at[way],
            device_id=at(o, 0),
            device_id_type=MESH,
        )

    def strip_copies(late):
        copies = [narrow_copy(late, o, dy) for dy in (-1, 1) for o in near]
        copies += [wide_copy(late, o) for o in (-1, 1)]
        if late:
            copies += [far_copy(0, -2), far_copy(1, 2)]
        return copies

    def pack_wide(items, index):
        parts = []
        for p, v in enumerate(items):
            parts.append((within(32 * p, SLOT), lrl(v, 32 * p)))
            spot = (32 * p + 48) % 128
            parts.append((within(spot, SLOT), lrl(v, spot - (128 - OWNED))))
        wide[1, index] = overlay(parts)

    def pack_narrow(rows, index):
        upps, lows = [], []
        for i, items in enumerate(rows):
            for p, v in enumerate(items):
                spot = 32 * p + 8 * i
                upps.append((within(spot, 8), lrl(v, spot - (128 - GHOSTS))))
                lows.append((within(spot, 8), lrl(v, spot)))
        narrow[0, index] = overlay(upps)
        narrow[1, index] = overlay(lows)

    def pack_field(ref, wide_at, narrow_at):
        rows = [[tile(ref, a, p) for p in range(PAIRS)] for a in range(P_SIZE)]
        for a in range(P_SIZE):
            pack_wide(rows[a], wide_at + a)
        for q in range(2):
            pack_narrow(rows[4 * q:4 * q + 4], narrow_at + q)

    def pack_small():
        items = [small[f] for f in range(4)]
        pack_wide(items, 2 * P_SIZE)
        pack_narrow([items], PAIRS)

    def finish_first():
        for copy in y_copies():
            copy.wait_recv()
        cy = halves(yrecv[0], yrecv[1])
        first = bas.at[0]
        for a in range(P_SIZE):
            term = small[3] * jnp.where(edge_lane, lrl(cy, -a), 0.0)
            put(first, a, 0, tile(first, a, 0) + jnp.where(low, term, 0.0))
            last = PAIRS - 1
            put(first, a, last, tile(first, a, last) + jnp.where(low, 0.0, term))
        cw, ce = pack_faces(xfaces(functools.partial(tile, first)))
        far_send[0] = cw
        far_send[1] = ce
        pack_field(first, 0, 0)
        for copy in strip_copies(True):
            copy.start()

    def unpack(wide_at, narrow_at, i, p):
        parts = []
        for j in range(3):
            mask = within(SLOT * (j + 1), OWNED) | within(64 + SLOT * j, OWNED)
            parts.append((mask, lrl(wide[j, wide_at], SLOT * (j + 1) - 32 * p)))
        for j in range(3):
            for side in range(2):
                spot = 64 * side + SLOT * j + OWNED
                v = lrl(narrow_in[side, j, narrow_at], spot - 32 * p - 8 * i)
                parts.append((within(spot, GHOSTS), v))
        return overlay(parts)

    def unpack_early():
        for a, p in tiles():
            value = unpack(P_SIZE + a, 2 + a // 4, a % 4, p)
            put(page_rea, a, p, value - shift)
        for f in range(4):
            page_small[f] = unpack(2 * P_SIZE, PAIRS, 0, f)

    def unpack_late():
        for a, p in tiles():
            put(page_a, a, p, unpack(a, a // 4, a % 4, p))

    def page_level(level):
        given, out = (page_a, page_b) if level % 2 else (page_b, page_a)
        get = functools.partial(tile, given)
        fields = [page_small[f] for f in range(4)]
        fw, fe = xfaces(get)
        if level == 1:
            cw, ce = far_in[0], far_in[1]
            skip = 128 - OWNED
            east = jnp.where(lane < 64, lrl(cw, 3 * SLOT), lrl(cw, 6 * SLOT - skip))
            west = jnp.where(lane < 64, lrl(ce, SLOT), lrl(ce, 4 * SLOT - skip))
            last = within(2 * SLOT + OWNED, SLOT) | within(6 * SLOT, SLOT)
            first = within(OWNED, SLOT) | within(4 * SLOT, SLOT)
        sides = {}
        for p in range(PAIRS):
            e, w = lrl(srl(fw[p], 3), -SLOT), lrl(srl(fe[p], 5), SLOT)
            if level == 1:
                e = jnp.where(last, srl(east, 3 - p), e)
                w = jnp.where(first, srl(west, -p), w)
            nb_e = jnp.where(xpos == 3, e, srl(fw[p], 7))
            nb_w = jnp.where(xpos == 0, w, srl(fe[p], 1))
            sides[0, p] = fw[p] - fields[1] * nb_w
            sides[P_SIZE - 1, p] = fe[p] - fields[2] * nb_e
        own, across = yfaces(get)

        def emit(a, p, value):
            put(out, a, p, value)
            south = lrl(value, -2 * SLOT)
            north = lrl(value, 128 - OWNED - 5 * SLOT)
            patch[level - 1, a * PAIRS + p] = jnp.where(lane < 64, south, north)

        apply(get, functools.partial(tile, page_rea), fields, sides, own, across, emit)

    edge = (lane < VECS) | (lane >= 128 - VECS)

    def patched(level, a, p, v):
        if level == 0:
            return v
        return jnp.where(edge, patch[level - 1, a * PAIRS + p], v)

    def finish_rows(ref, first, last):
        for p in range(PAIRS):
            put(ref, 0, p, tile(ref, 0, p) + first[p])
            put(ref, P_SIZE - 1, p, tile(ref, P_SIZE - 1, p) + last[p])

    loads[0].wait()
    get = functools.partial(tile, ini)
    faces = xfaces(get)
    given = yfaces(get)
    loads[5].wait()
    loads[6].wait()
    operate(get, faces, given, lambda a, p, v: put(bas.at[0], a, p, tile(src, a, p) - v))

    late = gy == ny - 1
    for step in range(VECS // 2):
        now, after = bas.at[2 * step], bas.at[2 * step + 1]
        fw, fe = xfaces(functools.partial(tile, now))
        if step == 0:
            send_halo(0, faces, (fw, fe), lambda: pl.semaphore_wait(barrier, n - 1))
            send_yfaces(given[1])
            pack_field(rea, P_SIZE, 2)
            pack_small()
            for copy in strip_copies(False):
                copy.start()
        else:
            send_halo(step, faces, (fw, fe))
        if step == 1:
            pl.when(jnp.logical_not(late))(finish_first)
            accs = [None] * 3
            for a, p in tiles():
                u, v = tile(bas.at[0], a, p), tile(bas.at[1], a, p)
                new = [u * u, u * v, v * v]
                accs = new if accs[0] is None else [s + t for s, t in zip(accs, new)]
            start_reduce(0, pack_sums(accs, 0))
        if step == 2:
            pl.when(late)(finish_first)
            for copy in strip_copies(False):
                copy.wait_recv()
            unpack_early()
        (first, last), extra = take_halo(step, 1.0 if step == 0 else -1.0)
        fw = [fw[p] + glow[0] * first[p] + glow[P_SIZE - 1] * last[p] for p in range(PAIRS)]
        fe = [fe[p] + gupp[0] * first[p] + gupp[P_SIZE - 1] * last[p] for p in range(PAIRS)]
        finish_rows(now, first, last)
        operate(functools.partial(tile, now), (fw, fe), None, functools.partial(put, after))
        finish_rows(after, *extra)
        if step < VECS // 2 - 1:
            get = functools.partial(tile, after)
            faces = xfaces(get)
            operate(get, faces, None, functools.partial(put, bas.at[2 * step + 2]))

    for copy in strip_copies(True):
        copy.wait_recv()
    unpack_late()
    for k in range(1, VECS):
        page_level(k)

    sums = end_reduce(0)
    size = jnp.maximum(sums(0), 1e-30)
    mean = sums(1) / size
    spread = jnp.sqrt(jnp.maximum(sums(2) / size - mean * mean, 0.0)) + 0.1
    inv = 1.0 / spread
    ratio = mean * inv
    theta = shift + mean
    powers = [None, inv]
    for k in range(2, VECS):
        powers.append(powers[k - 1] * inv)

    pairs = [(i, j) for j in range(VECS) for i in range(j + 1)]
    accs = None
    for a, p in tiles():
        lev = []
        for k in range(VECS):
            v = patched(k, a, p, tile(bas.at[k], a, p))
            lev.append(v if k == 0 else v * powers[k])
        vecs = [lev[0]]
        for k in range(1, VECS):
            lev = [lev[i + 1] - ratio * lev[i] for i in range(len(lev) - 1)]
            vecs.append(lev[0])
        for k in range(1, VECS):
            put(bas.at[k], a, p, vecs[k])
        new = [vecs[i] * vecs[j] for i, j in pairs]
        accs = new if accs is None else [s + t for s, t in zip(accs, new)]
    packed = pack_sums(accs[:8], 0) + pack_sums(accs[8:16], 8) + pack_sums(accs[16:], 16)
    start_reduce(1, packed)
    sums = end_reduce(1)

    gram = {}
    for k, (i, j) in enumerate(pairs):
        gram[i, j] = sums(k) * (1.0 / total)
    def times_gram(u, rows):
        return [
            dot((gram[min(i, r), max(i, r)], u[i]) for i in range(len(u))) for r in range(rows)
        ]

    hess = jnp.zeros((8, 128), jnp.float32)
    combos = [[1.0 / jnp.sqrt(gram[0, 0] + FLOOR)]]
    for j in range(ITERS):
        c = combos[j]
        u = [theta * c[0]]
        for i in range(1, j + 1):
            u.append(spread * c[i - 1] + theta * c[i])
        u.append(spread * c[j])
        g = times_gram(u, j + 1)
        rest = list(u)
        for i in range(j + 1):
            h = dot(zip(combos[i], g))
            hess = jnp.where((sub == i) & (lane == j), h, hess)
            for k in range(i + 1):
                rest[k] = rest[k] - h * combos[i][k]
        square = dot(zip(rest, times_gram(rest, j + 2)))
        beta = jnp.sqrt(jnp.maximum(square, 0.0) + FLOOR)
        hess = jnp.where((sub == j + 1) & (lane == j), beta, hess)
        post = 1.0 / beta
        combos.append([r * post for r in rest])

    for a, p in tiles():
        vecs = [tile(bas.at[k], a, p) for k in range(VECS)]
        for j in reversed(range(VECS)):
            put(bas.at[j], a, p, dot(zip(combos[j], vecs)))
    hess_out[...] = hess[0:VECS, 0:ITERS]

    halos = [copy for slot in range(VECS // 2) for copy in halo_copies(slot)]
    for copy in halos + y_copies() + [far_copy(0, -2), far_copy(1, 2)]:
        copy.wait_send()
    for block, sem in ((narrow_in, ns_sem), (wide.at[pl.ds(0, 2)], ws_sem)):
        pltpu.make_async_copy(block, block, sem.at[0]).wait()
    for slot in range(2):
        block = rrecv.at[slot, pl.ds(0, n - 1)]
        pltpu.make_async_copy(block, block, rs_sem.at[slot]).wait()


def store(hess, basis, hess_out, basis_out, sem):
    copies = [
        pltpu.make_async_copy(basis, basis_out, sem.at[0]),
        pltpu.make_async_copy(hess, hess_out, sem.at[1]),
    ]
    for copy in copies:
        copy.start()
    for copy in copies:
        copy.wait()


def body(nx, ny, source, initial, reaction, stiffness, line_op, face_deriv, wall_flags):
    nodes, ex, ey = source.shape
    n = nx * ny
    rows = nodes * ex
    flat = (rows, ey)
    total = float(nodes * ex * nx * ey * ny)
    vmem = pl.BlockSpec(memory_space=pltpu.VMEM)
    hbm = pl.BlockSpec(memory_space=pl.ANY)

    def array(*lead):
        return pltpu.VMEM(lead + (8, 128), jnp.float32)

    dma = pltpu.SemaphoreType.DMA
    hess, basis = pl.pallas_call(
        functools.partial(kernel, nx, ny, total),
        out_shape=(
            pltpu.VMEM((VECS, ITERS), jnp.float32),
            pltpu.VMEM((VECS,) + flat, jnp.float32),
        ),
        in_specs=[hbm] * 7,
        out_specs=(vmem, vmem),
        scratch_shapes=[
            pltpu.SMEM(line_op.shape, jnp.float32),
            pltpu.SMEM(face_deriv.shape, jnp.float32),
            pltpu.VMEM(stiffness.shape, jnp.float32),
            pltpu.VMEM(wall_flags.shape, wall_flags.dtype),
            array(2 * PAIRS * PAIRS),
            array(2 * PAIRS),
            array(4),
            pltpu.VMEM(flat, jnp.float32),
            pltpu.VMEM(flat, jnp.float32),
            pltpu.VMEM(flat, jnp.float32),
            array(3, WIDE),
            array(2, NARROW),
            array(2, 3, NARROW),
            array(2),
            array(2),
            pltpu.VMEM(flat, jnp.float32),
            array(4),
            pltpu.VMEM(flat, jnp.float32),
            pltpu.VMEM(flat, jnp.float32),
            array(ITERS, P_SIZE * PAIRS),
            dma((7,)),
            array(VECS // 2, 2, 3),
            array(VECS // 2, 2, 3),
            array(),
            array(2),
            pltpu.VMEM((2, 1, 128), jnp.float32),
            pltpu.VMEM((2, n, 128), jnp.float32),
            dma((VECS // 2, 2)),
            dma((VECS // 2, 2)),
            dma((2,)),
            dma((2,)),
            dma((1,)),
            dma((2, 3)),
            dma((1,)),
            dma((2, 2, 3)),
            dma((2,)),
            dma((2,)),
            dma((2,)),
            dma((2,)),
        ],
        compiler_params=pltpu.CompilerParams(collective_id=0, has_side_effects=True),
    )(
        line_op, face_deriv, source.reshape(flat), initial.reshape(flat), reaction.reshape(flat),
        stiffness, wall_flags,
    )
    hess = pltpu.with_memory_space_constraint(hess, pltpu.VMEM)
    basis = pltpu.with_memory_space_constraint(basis, pltpu.VMEM)
    hess, basis = pl.pallas_call(
        store,
        out_shape=(
            jax.ShapeDtypeStruct(hess.shape, jnp.float32),
            jax.ShapeDtypeStruct(basis.shape, jnp.float32),
        ),
        in_specs=[hbm, hbm],
        out_specs=(hbm, hbm),
        scratch_shapes=[pltpu.SemaphoreType.DMA((2,))],
    )(hess, basis)
    return hess, basis.reshape((VECS, nodes, ex, ey))


def solution(mesh):
    return jax.shard_map(
        functools.partial(body, mesh.shape["gx"], mesh.shape["gy"]),
        mesh=mesh,
        in_specs=(
            P(None, "gx", "gy"),
            P(None, "gx", "gy"),
            P(None, "gx", "gy"),
            P("gx", "gy"),
            P(),
            P(),
            P(None, "gx", "gy"),
        ),
        out_specs=(P(), P(None, None, "gx", "gy")),
        check_vma=False,
    )
```
